256 devices in a mesh: gx: 8 (over y, x_lo), gy: 4 (over x_hi, core), gz: 8 (over z).
Axes of the slice: x: 4 (x_hi: 2, x_lo: 2; x = x_hi * 2 + x_lo), y: 4, z: 8, core: 2. Of those that a mesh axis runs over, the one named last changes fastest.
Arguments:
- occupancy: int32 [128, 256, 1024], P('gx', 'gy', 'gz'), may hold values 0 or 1
- site_field: float32 [128, 256, 1024], P('gx', 'gy', 'gz'), may hold values from -6 to 6
- attempt_rate: float32 [128, 256, 1024], P('gx', 'gy', 'gz'), may hold values from 0.2 to 5
- uniforms: float32 [8, 128, 256, 512], P(None, 'gx', 'gy', 'gz'), may hold values from 0.001 to 1
Outputs:
- final_spins: float32 [128, 256, 1024], P('gx', 'gy', 'gz')
- history: float32 [2, 8], replicated
The draws below stay inside these ranges and needn't reach their ends.
All inputs are finite; a program needn't handle non-finite values. No bound on the sum of `occupancy` on one device may be relied on, other than what follows from the above.
Results may differ from the reference program's by a relative error of at most 0.0002.
Values sent between devices are 32-bit elements; how exact they have to be, the bound alone decides.
No kernel may reach another device: no remote copies, remote signals or barrier semaphores. Data moves between devices by JAX's collectives and lax.ppermute only.
A program may use at most 128 MiB of HBM per device.

```python
import math
import jax
import jax.numpy as jnp
from jax import lax

SECTIONS = 8
NX = 128
NY = 256
NZ = 1024


def place_ends(values, rng, least, largest):
    longest = values.shape.index(max(values.shape))
    spots = []
    for shift in (0, 1):
        where = [jax.random.randint(jax.random.fold_in(rng, axis), (), 0, length) for axis, length in enumerate(values.shape)]
        where[longest] = (where[longest] + shift) % values.shape[longest]
        spots.append(tuple(where))
    return values.at[spots[0]].set(least).at[spots[1]].set(largest)


def level_of(key, shape, cuts, smallest, largest):
    loudness, own = 1.0, jax.random.fold_in(key, 6)
    for dim, blocks in cuts:
        heights = jnp.exp(jax.random.uniform(jax.random.fold_in(own, dim), (blocks,), jnp.float32, smallest / len(cuts), largest / len(cuts)))
        loudness = loudness * jnp.repeat(heights, shape[dim] // blocks).reshape([-1 if axis == dim else 1 for axis in range(len(shape))])
    return loudness


def bell_draw(rng, extent, width, most, shards=(), held_as=jnp.bfloat16):
    array = jax.random.normal(rng, extent, jnp.float32) * width
    if len(shards) > 0:
        array = level_of(rng, extent, shards, -0.22, 0.18) * array
    return jnp.clip(array, min=-most, max=most).astype(held_as)


def setup_inputs(seed: int = 0) -> dict:
    key_of = jax.random.split(jax.random.key(seed), 5)
    occupancy = place_ends((jax.random.randint(key_of[0], (NX, NY, NZ), 0, 2) < 1).astype(jnp.int32), jax.random.fold_in(key_of[0], 1), 0, 1)
    site_field = bell_draw(key_of[1], (NX, NY, NZ), 1.0, 6.0, ((0, 8), (1, 4), (2, 8)), jnp.float32)
    attempt_rate = jnp.clip(jnp.exp(math.log(5.0) - 3.218876 * jax.random.uniform(key_of[2], (NX, NY, NZ), jnp.float32) ** level_of(key_of[2], (NX, NY, NZ), ((0, 8), (1, 4), (2, 8)), -0.2, 0.2)), 0.2, 5.0)
    uniforms = jnp.clip(0.001 + 0.999 * jax.random.uniform(key_of[3], (SECTIONS, NX, NY, NZ // 2), jnp.float32) ** level_of(key_of[3], (SECTIONS, NX, NY, NZ // 2), ((1, 8), (2, 4), (3, 8)), -0.2, 0.2), 0.001, 1.0)
    return dict(occupancy=occupancy, site_field=site_field, attempt_rate=attempt_rate, uniforms=uniforms)


coupling = 0.5
softness = 0.5


def neighbours(spin):
    total = jnp.roll(spin, 1, 0) + jnp.roll(spin, -1, 0)
    total = total + jnp.roll(spin, 1, 1) + jnp.roll(spin, -1, 1)
    return total + jnp.roll(spin, 1, 2) + jnp.roll(spin, -1, 2)


def parity_mask(shape, phase):
    xpos = lax.broadcasted_iota(jnp.int32, shape, 0)
    ypos = lax.broadcasted_iota(jnp.int32, shape, 1)
    zpos = lax.broadcasted_iota(jnp.int32, shape, 2)
    return (((xpos + ypos + zpos) % 2) == phase).astype(jnp.float32)


def unpack_draws(packed, phase):
    shape = packed.shape
    xpos = lax.broadcasted_iota(jnp.int32, shape, 0)
    ypos = lax.broadcasted_iota(jnp.int32, shape, 1)
    select = (xpos + ypos + phase) % 2
    first = jnp.where(select == 0, packed, jnp.float32(1.0))
    second = jnp.where(select == 1, packed, jnp.float32(1.0))
    return jnp.stack([first, second], -1).reshape(shape[0], shape[1], 2 * shape[2])


def reference(occupancy, site_field, attempt_rate, uniforms):
    spin = 2.0 * occupancy.astype(jnp.float32) - 1.0
    sites_total = spin.size
    half_sites = sites_total / 2.0
    clock = jnp.float32(0.0)
    energies = []
    times = []
    for section_index in range(SECTIONS):
        phase = section_index % 2
        mask = parity_mask(spin.shape, phase)
        beside_all = neighbours(spin)
        delta = 2.0 * spin * (site_field - coupling * beside_all)
        rate_log = jnp.log(attempt_rate) - jax.nn.softplus(delta)
        total_rate = jnp.sum(mask * jnp.exp(rate_log))
        log_dt = jnp.log(jnp.float32(half_sites)) - jnp.log(total_rate)
        draws_full = unpack_draws(uniforms[section_index], phase)
        accept = jax.nn.sigmoid((rate_log + log_dt - jnp.log(draws_full)) / softness)
        spin = spin - 2.0 * accept * spin * mask
        energy = (coupling * jnp.sum(mask * spin * beside_all) - jnp.sum(site_field * spin)) / sites_total
        clock = clock + half_sites / total_rate
        energies.append(energy)
        times.append(clock)
    history = jnp.stack([jnp.stack(energies), jnp.stack(times)]).astype(jnp.float32)
    return spin, history
```

```python
import functools

import jax
import jax.numpy as jnp
from jax import lax
from jax.experimental import pallas as pl
from jax.experimental.pallas import tpu as pltpu
from jax.sharding import PartitionSpec as P

SECTIONS = 8
AXES = ("gx", "gy", "gz")
BX, BY, BZ = 16, 64, 128
HY, HZ = BY // 2, BZ // 2
LEFT = 8
F32 = jnp.float32


def lane_of(rows=HY):
    return lax.broadcasted_iota(jnp.int32, (rows, BZ), 1)


def odd_row(shift, rows=HY):
    return (lax.broadcasted_iota(jnp.int32, (rows, BZ), 0) + shift) % 2 == 1


def roll(value, shift):
    shift = shift % BZ
    return value if shift == 0 else pltpu.roll(value, shift, 1)


def shuffle_matrix(transposed):
    major = lax.broadcasted_iota(jnp.int32, (BZ, BZ), 1 if transposed else 0)
    minor = lax.broadcasted_iota(jnp.int32, (BZ, BZ), 0 if transposed else 1)
    return (minor == major // 2 + HZ * (major % 2)).astype(F32)


def matmul(a, b, exact):
    precision = lax.Precision.HIGHEST if exact else lax.Precision.DEFAULT
    return jnp.dot(a, b, precision=precision, preferred_element_type=F32)


def face_column(plane, x, phase):
    ends = jnp.where(odd_row(x + phase), roll(plane, HZ + 1), plane)
    return roll(ends, x)


def pack_kernel(occ, field, attempt, spin, h, a, xlo, xhi, ylo, yhi, zed):
    lane = lane_of()
    low = lane < HZ
    wide = shuffle_matrix(False)
    for x in range(BX):
        odd = odd_row(x)
        for source, exact, kind in ((occ, False, 0), (field, True, 1), (attempt, True, 2)):
            plane = source[x]
            if kind == 0:
                plane = 2.0 * plane.astype(F32) - 1.0
            mixed = matmul(plane, wide, exact)
            lower, upper = mixed[:HY], mixed[HY:]
            lower_turned, upper_turned = roll(lower, HZ), roll(upper, HZ)
            even_site = jnp.where(low, jnp.where(odd, lower_turned, lower), jnp.where(odd, upper, upper_turned))
            odd_site = jnp.where(low, jnp.where(odd, lower, lower_turned), jnp.where(odd, upper_turned, upper))
            if kind == 0:
                spin[0, x + 1, LEFT : LEFT + HY] = even_site
                spin[1, x + 1, LEFT : LEFT + HY] = odd_site
            else:
                target = h if kind == 1 else a
                target[0, x] = even_site
                target[1, x] = odd_site
    for p in range(2):
        column = jnp.zeros((HY, BZ), F32)
        xlo[p] = spin[p, 1, LEFT : LEFT + HY]
        xhi[p] = spin[p, BX, LEFT : LEFT + HY]
        for x in range(BX):
            plane = spin[p, x + 1, LEFT : LEFT + HY]
            ylo[p, x : x + 1] = plane[:1]
            yhi[p, x : x + 1] = plane[HY - 1 :]
            column = jnp.where(lane % HZ == x, face_column(plane, x, p), column)
        zed[p] = column


def draws_kernel(uniforms, a, v):
    for k in range(SECTIONS):
        for x in range(BX):
            both = jnp.concatenate([uniforms[k, x, :HY], uniforms[k, x, HY:]], axis=1)
            v[k, x] = both / a[k % 2, x]


def z_parts(phase):
    lane = lane_of()
    row = lax.broadcasted_iota(jnp.int32, (HY, BZ), 0)
    return (lane % HZ + row + phase) % 2 == 1


def flip_of(total, half):
    ratio = total / half
    square = ratio * ratio
    return lambda odds: 1.0 - 2.0 / (1.0 + odds * square)


def eighth(value):
    return value[0:8] + value[8:16] + value[16:24] + value[24:32]


def advance(k, half, gathered, halo, spin, side, column, odds, gain, h, energy, fields, clock):
    p = (k - 1) % 2
    total = jnp.sum(jnp.sum(gathered[...], axis=0, keepdims=True), axis=1, keepdims=True)
    flip = flip_of(total, half)
    elapsed = clock[1:2, :] + half / total
    clock[1:2, :] = elapsed
    clock[0:1, :] = jnp.where(lane_of(1) == k - 1, elapsed, clock[0:1, :])
    of_gain = jnp.zeros((HY, BZ), F32)
    of_field = jnp.zeros((HY, BZ), F32)
    for x in range(BX):
        new = spin[p, x + 1, LEFT : LEFT + HY] * flip(odds[x])
        spin[p, x + 1, LEFT : LEFT + HY] = new
        of_gain = of_gain + new * gain[x]
        of_field = of_field + new * h[p, x]
    fields[p] = eighth(of_field)
    energy[k - 1] = -eighth(of_gain) - fields[1 - p]
    if halo is None:
        return
    from_xlo, from_xhi, from_ylo, from_yhi, from_zlo, from_zhi = halo
    spin[p, 0, LEFT : LEFT + HY] = spin[p, 0, LEFT : LEFT + HY] * flip(from_xlo[...])
    spin[p, BX + 1, LEFT : LEFT + HY] = spin[p, BX + 1, LEFT : LEFT + HY] * flip(from_xhi[...])
    side[p] = side[p] * flip(jnp.where(lane_of(BX) < HZ, from_yhi[...], from_ylo[...]))
    column[p] = column[p] * flip(jnp.where(z_parts(p), from_zlo[...], from_zhi[...]))


def rates(k, spin, side, column, odds, gain, h, a, v, xlo, xhi, ylo, yhi, zed, sent):
    act, p = k % 2, 1 - k % 2
    lane = lane_of()
    one_row = lane_of(1)
    for x in range(BX):
        first, last = spin[p, x + 1, LEFT : LEFT + 1], spin[p, x + 1, LEFT + HY - 1 : LEFT + HY]
        beyond = side[p, x : x + 1]
        spin[p, x + 1, LEFT - 1 : LEFT] = roll(jnp.where(one_row < HZ, last, beyond), HZ)
        spin[p, x + 1, LEFT + HY : LEFT + HY + 1] = roll(jnp.where(one_row < HZ, beyond, first), HZ)
    ends = column[p]
    packed = jnp.zeros((HY, BZ), F32)
    summed = jnp.zeros((HY, BZ), F32)
    for x in range(BX):
        odd = odd_row(x + act)
        here = spin[p, x + 1, LEFT : LEFT + HY]
        turned = jnp.where(odd, roll(here, -1), roll(here, 1))
        edge = jnp.where(odd, roll(ends, HZ - 1 - x), roll(ends, -x))
        at_edge = lane % HZ == jnp.where(odd, HZ - 1, 0)
        beside = spin[p, x, LEFT : LEFT + HY] + spin[p, x + 2, LEFT : LEFT + HY]
        beside = beside + spin[p, x + 1, LEFT - 1 : LEFT + HY - 1] + spin[p, x + 1, LEFT + 1 : LEFT + HY + 1]
        beside = beside + here + jnp.where(at_edge, edge, turned)
        g = h[act, x] - 0.5 * beside
        gain[x] = g
        grown = 1.0 + jnp.exp(2.0 * spin[act, x + 1, LEFT : LEFT + HY] * g)
        summed = summed + a[act, x] / grown
        root = v[x] * grown
        square = root * root
        odds[x] = square
        ylo[x : x + 1] = square[:1]
        yhi[x : x + 1] = square[HY - 1 :]
        packed = jnp.where(lane % HZ == x, face_column(square, x, act), packed)
        if x == 0:
            xlo[...] = square
        if x == BX - 1:
            xhi[...] = square
    zed[...] = packed
    sent[...] = jnp.broadcast_to(jnp.sum(summed, axis=0, keepdims=True), sent.shape)


def first_kernel(
    from_xlo, from_xhi, from_ylo, from_yhi, from_zlo, from_zhi, h, a, v, spin_in,
    spin, side, column, energy, fields, clock, odds, gain, xlo, xhi, ylo, yhi, zed, sent,
):
    for p in range(2):
        spin[p, 0, LEFT : LEFT + HY] = from_xlo[p]
        spin[p, BX + 1, LEFT : LEFT + HY] = from_xhi[p]
        side[p] = jnp.where(lane_of(BX) < HZ, from_yhi[p], from_ylo[p])
        column[p] = jnp.where(z_parts(p), from_zlo[p], from_zhi[p])
    of_field = jnp.zeros((HY, BZ), F32)
    for x in range(BX):
        of_field = of_field + spin[1, x + 1, LEFT : LEFT + HY] * h[1, x]
    fields[0] = jnp.zeros((8, BZ), F32)
    fields[1] = eighth(of_field)
    energy[...] = jnp.zeros(energy.shape, F32)
    clock[...] = jnp.zeros(clock.shape, F32)
    rates(0, spin, side, column, odds, gain, h, a, v.at[0], xlo, xhi, ylo, yhi, zed, sent)


def section_kernel(
    k, half, gathered, from_xlo, from_xhi, from_ylo, from_yhi, from_zlo, from_zhi, h, a, v,
    spin_in, side_in, column_in, energy_in, fields_in, clock_in, odds_in, gain_in,
    spin, side, column, energy, fields, clock, odds, gain, xlo, xhi, ylo, yhi, zed, sent,
):
    halo = (from_xlo, from_xhi, from_ylo, from_yhi, from_zlo, from_zhi)
    advance(k, half, gathered, halo, spin, side, column, odds, gain, h, energy, fields, clock)
    rates(k, spin, side, column, odds, gain, h, a, v.at[k], xlo, xhi, ylo, yhi, zed, sent)


def last_kernel(
    half, gathered, h, odds, gain, spin_in, energy_in, fields_in, clock_in,
    spin, energy, fields, clock, sent,
):
    advance(SECTIONS, half, gathered, None, spin, None, None, odds, gain, h, energy, fields, clock)
    row = jnp.zeros((1, BZ), F32)
    for k in range(SECTIONS):
        value = jnp.sum(jnp.sum(energy[k], axis=0, keepdims=True), axis=1, keepdims=True)
        row = jnp.where(lane_of(1) == k, value, row)
    sent[...] = jnp.broadcast_to(row, sent.shape)


def unpack_kernel(spin, out):
    low = lane_of() < HZ
    narrow = shuffle_matrix(True)
    for x in range(BX):
        even_site, odd_site = spin[0, x + 1, LEFT : LEFT + HY], spin[1, x + 1, LEFT : LEFT + HY]
        odd = odd_row(x)
        even_z, odd_z = jnp.where(odd, odd_site, even_site), jnp.where(odd, even_site, odd_site)
        lower = jnp.where(low, even_z, roll(odd_z, HZ))
        upper = jnp.where(low, roll(even_z, HZ), odd_z)
        out[x, :HY] = matmul(lower, narrow, True)
        out[x, HY:] = matmul(upper, narrow, True)


def history_kernel(sites, gathered, clock, out):
    row = jnp.sum(gathered[...], axis=0, keepdims=True) / sites
    out[0:1, :] = row[:, :SECTIONS]
    out[1:2, :] = clock[0:1, :SECTIONS]


def call(kernel, name, inputs, outputs, aliases=None, flops=1000000):
    vmem = pl.BlockSpec(memory_space=pltpu.VMEM)
    return pl.pallas_call(
        kernel,
        name=name,
        out_shape=[jax.ShapeDtypeStruct(shape, F32) for shape in outputs],
        in_specs=[vmem] * len(inputs),
        out_specs=[vmem] * len(outputs),
        input_output_aliases=aliases or {},
        compiler_params=pltpu.CompilerParams(vmem_limit_bytes=32 * 1024 * 1024),
        cost_estimate=pl.CostEstimate(flops=flops, bytes_accessed=1000000, transcendentals=0),
    )(*inputs)


def swap(xlo, xhi, ylo, yhi, zlo, zhi):
    got = []
    for axis, low, high in (("gx", xlo, xhi), ("gy", ylo, yhi), ("gz", zlo, zhi)):
        count = lax.axis_size(axis)
        up = [(i, (i + 1) % count) for i in range(count)]
        got.append(lax.ppermute(high, axis, up))
        got.append(lax.ppermute(low, axis, [(b, a) for a, b in up]))
    return got


def spread(sent):
    return lax.all_to_all(sent, AXES, 0, 0, tiled=True)


def body(occupancy, site_field, attempt_rate, uniforms):
    devices = lax.axis_size(AXES)
    sites = float(BX * BY * BZ * devices)
    half = sites / 2.0
    tile = (HY, BZ)
    spin_shape = (2, BX + 2, HY + 2 * LEFT, BZ)
    block = (BX, *tile)
    faces = [tile, tile, (BX, BZ), (BX, BZ), tile]
    state = [spin_shape, (2, BX, BZ), (2, *tile), (SECTIONS, 8, BZ), (2, 8, BZ), (8, BZ), block, block]
    sent_shape = (devices, BZ)
    spin, h, a, xlo, xhi, ylo, yhi, zed = call(
        pack_kernel, "pack", (occupancy, site_field, attempt_rate),
        [spin_shape, (2, *block), (2, *block)] + [(2, *face) for face in faces],
    )
    halo = swap(xlo, xhi, ylo, yhi, zed, zed)
    (v,) = call(draws_kernel, "draws", (uniforms, a), [(SECTIONS, *block)])
    carried = call(
        first_kernel, "section0", (*halo, h, a, v, spin), state + faces + [sent_shape], {9: 0},
    )
    for k in range(1, SECTIONS):
        *kept, xlo, xhi, ylo, yhi, zed, sent = carried
        halo = swap(xlo, xhi, ylo, yhi, zed, zed)
        gathered = spread(sent)
        carried = call(
            functools.partial(section_kernel, k, half), f"section{k}",
            (gathered, *halo, h, a, v, *kept), state + faces + [sent_shape],
            {10 + i: i for i in range(len(state))},
        )
    spin, _, _, energy, fields, clock, odds, gain = carried[: len(state)]
    gathered = spread(carried[-1])
    spin, energy, fields, clock, sent = call(
        functools.partial(last_kernel, half), "last",
        (gathered, h, odds, gain, spin, energy, fields, clock),
        [spin_shape, state[3], state[4], state[5], sent_shape], {4: 0, 5: 1, 6: 2, 7: 3},
    )
    gathered = spread(sent)
    (final,) = call(unpack_kernel, "unpack", (spin,), [(BX, BY, BZ)])
    (history,) = call(
        functools.partial(history_kernel, sites), "history", (gathered, clock), [(2, SECTIONS)],
    )
    return final, history


def solution(mesh):
    return jax.shard_map(
        body,
        mesh=mesh,
        in_specs=(P(*AXES), P(*AXES), P(*AXES), P(None, *AXES)),
        out_specs=(P(*AXES), P()),
        check_vma=False,
    )
```

```python
import functools

import jax
import jax.numpy as jnp
from jax import lax
from jax.experimental import pallas as pl
from jax.experimental.pallas import tpu as pltpu
from jax.sharding import PartitionSpec as P

SECTIONS = 8
AXES = ("gx", "gy", "gz")
BX, BY, BZ = 16, 64, 128
HY, HZ = BY // 2, BZ // 2
UNROLL = 4
CHUNK = 4
PITCH = HY + 8
F32 = jnp.float32


def lane_of(rows=HY):
    return lax.broadcasted_iota(jnp.int32, (rows, BZ), 1)


def odd_row(shift, rows=HY):
    return (lax.broadcasted_iota(jnp.int32, (rows, BZ), 0) + shift) % 2 == 1


def roll(value, shift):
    shift = shift % BZ
    return value if shift == 0 else pltpu.roll(value, shift, 1)


def shuffle_matrix(transposed):
    major = lax.broadcasted_iota(jnp.int32, (BZ, BZ), 1 if transposed else 0)
    minor = lax.broadcasted_iota(jnp.int32, (BZ, BZ), 0 if transposed else 1)
    return (minor == major // 2 + HZ * (major % 2)).astype(F32)


def matmul(a, b, exact):
    precision = lax.Precision.HIGHEST if exact else lax.Precision.DEFAULT
    return jnp.dot(a, b, precision=precision, preferred_element_type=F32)


def face_column(plane, x, phase):
    ends = jnp.where(odd_row(x + phase), roll(plane, HZ + 1), plane)
    return roll(ends, x)


def fetch(pairs, arrived):
    copies = [pltpu.make_async_copy(source, target, arrived.at[i]) for i, (source, target) in enumerate(pairs)]
    for copy in copies:
        copy.start()
    return copies


def split_sites(mixed, odd, low):
    lower, upper = mixed[:HY], mixed[HY:]
    lower_turned, upper_turned = roll(lower, HZ), roll(upper, HZ)
    even_site = jnp.where(low, jnp.where(odd, lower_turned, lower), jnp.where(odd, upper, upper_turned))
    odd_site = jnp.where(low, jnp.where(odd, lower, lower_turned), jnp.where(odd, upper_turned, upper))
    return even_site, odd_site


def spins_kernel(occ_hbm, spin, xlo, xhi, ylo, yhi, zed, occ, arrived):
    copies = fetch([(occ_hbm.at[pl.ds(c * CHUNK, CHUNK)], occ.at[pl.ds(c * CHUNK, CHUNK)]) for c in range(BX // CHUNK)], arrived)
    lane = lane_of()
    wide = shuffle_matrix(False)
    columns = [jnp.zeros((HY, BZ), F32)] * 2
    for x in range(BX):
        if x % CHUNK == 0:
            copies[x // CHUNK].wait()
        planes = split_sites(matmul(2.0 * occ[x].astype(F32) - 1.0, wide, False), odd_row(x), lane < HZ)
        for p, plane in enumerate(planes):
            spin[p, x + 1, :HY] = plane
            ylo[p, x : x + 1] = plane[:1]
            yhi[p, x : x + 1] = plane[HY - 1 :]
            columns[p] = jnp.where(lane % HZ == x, face_column(plane, x, p), columns[p])
            if x == 0:
                xlo[p] = plane
            if x == BX - 1:
                xhi[p] = plane
    for p in range(2):
        zed[p] = columns[p]


def fields_kernel(
    field_hbm, attempt_hbm, uniforms, h, a_out, v_out, field, attempt, raw, a, v, arrived, drawn, left,
):
    copies = fetch([(field_hbm, field), (attempt_hbm, attempt)], arrived)
    draws = fetch([(uniforms.at[k], raw.at[k]) for k in range(SECTIONS)], drawn)
    low = lane_of() < HZ
    wide = shuffle_matrix(False)
    for copy in copies:
        copy.wait()

    @pl.loop(0, BX // UNROLL)
    def _(i):
        for j in range(UNROLL):
            x = i * UNROLL + j
            h[0, x], h[1, x] = split_sites(matmul(field[x], wide, True), odd_row(j), low)
            a[0, x], a[1, x] = split_sites(matmul(attempt[x], wide, True), odd_row(j), low)

    writes = [pltpu.make_async_copy(a, a_out, left.at[SECTIONS])]
    writes[0].start()
    for k in range(SECTIONS):
        draws[k].wait()

        @pl.loop(0, BX // UNROLL)
        def _(i):
            for j in range(UNROLL):
                x = i * UNROLL + j
                v[k, x] = jnp.concatenate([raw[k, x, :HY], raw[k, x, HY:]], axis=1) / a[k % 2, x]

        write = pltpu.make_async_copy(v.at[k], v_out.at[k], left.at[k])
        write.start()
        writes.append(write)
    for write in writes:
        write.wait()


def z_parts(phase):
    lane = lane_of()
    row = lax.broadcasted_iota(jnp.int32, (HY, BZ), 0)
    return (lane % HZ + row + phase) % 2 == 1


def flip_of(total, half):
    ratio = total / half
    square = ratio * ratio
    return lambda odds: 1.0 - 2.0 / (1.0 + odds * square)


def eighth(value):
    return value[0:8] + value[8:16] + value[16:24] + value[24:32]


def advance(k, p, half, gathered, halo, spin, side, column, odds, gain, h, energy, fields, clock):
    total = jnp.sum(jnp.sum(gathered[...], axis=0, keepdims=True), axis=1, keepdims=True)
    flip = flip_of(total, half)
    elapsed = clock[1:2, :] + half / total
    clock[1:2, :] = elapsed
    clock[0:1, :] = jnp.where(lane_of(1) == k - 1, elapsed, clock[0:1, :])
    of_gain = jnp.zeros((HY, BZ), F32)
    of_field = jnp.zeros((HY, BZ), F32)

    def step(i, carry):
        of_gain, of_field = carry
        for j in range(UNROLL):
            x = i * UNROLL + j
            new = spin[p, x + 1, :HY] * flip(odds[x])
            spin[p, x + 1, :HY] = new
            of_gain = of_gain + new * gain[x]
            of_field = of_field + new * h[p, x]
        return of_gain, of_field

    of_gain, of_field = lax.fori_loop(0, BX // UNROLL, step, (of_gain, of_field))
    fields[p] = eighth(of_field)
    energy[k - 1] = -eighth(of_gain) - fields[1 - p]
    if halo is None:
        return
    from_xlo, from_xhi, from_ylo, from_yhi, from_zlo, from_zhi = halo
    spin[p, 0, :HY] = spin[p, 0, :HY] * flip(from_xlo[...])
    spin[p, BX + 1, :HY] = spin[p, BX + 1, :HY] * flip(from_xhi[...])
    side[p] = side[p] * flip(jnp.where(lane_of(BX) < HZ, from_yhi[...], from_ylo[...]))
    column[p] = column[p] * flip(jnp.where(z_parts(p), from_zlo[...], from_zhi[...]))


def rates(act, spin, side, column, odds, gain, h, a, v, xlo, xhi, ylo, yhi, zed, sent):
    p = 1 - act
    lane = lane_of()
    one_row = lane_of(1)
    for x in range(BX):
        first, last = spin[p, x + 1, :1], spin[p, x + 1, HY - 1 : HY]
        beyond = side[p, x : x + 1]
        spin[p, x + 1, HY + 1 : HY + 2] = roll(jnp.where(one_row < HZ, last, beyond), HZ)
        spin[p, x + 1, HY : HY + 1] = roll(jnp.where(one_row < HZ, beyond, first), HZ)
    ends = column[p]
    top = lax.broadcasted_iota(jnp.int32, (HY, BZ), 0) == 0

    def step(i, carry):
        packed, summed = carry
        for j in range(UNROLL):
            x = i * UNROLL + j
            odd = odd_row(j + act)
            here = spin[p, x + 1, :HY]
            turned = jnp.where(odd, roll(here, -1), roll(here, 1))
            edge = jnp.where(odd, pltpu.roll(ends, (HZ - 1 - x) % BZ, 1), pltpu.roll(ends, (BZ - x) % BZ, 1))
            at_edge = lane % HZ == jnp.where(odd, HZ - 1, 0)
            beside = spin[p, x, :HY] + spin[p, x + 2, :HY]
            beside = beside + jnp.where(top, spin[p, x + 1, HY + 1 : HY + 2], pltpu.roll(here, 1, 0)) + spin[p, x + 1, 1 : HY + 1]
            beside = beside + here + jnp.where(at_edge, edge, turned)
            g = h[act, x] - 0.5 * beside
            gain[x] = g
            grown = 1.0 + jnp.exp(2.0 * spin[act, x + 1, :HY] * g)
            summed = summed + a[x] / grown
            root = v[x] * grown
            square = root * root
            odds[x] = square
            marked = jnp.where(odd, roll(square, HZ + 1), square)
            packed = jnp.where(lane % HZ == x, pltpu.roll(marked, x, 1), packed)
        return packed, summed

    packed, summed = lax.fori_loop(0, BX // UNROLL, step, (jnp.zeros((HY, BZ), F32), jnp.zeros((HY, BZ), F32)))
    xlo[...] = odds[0]
    xhi[...] = odds[BX - 1]
    for x in range(BX):
        ylo[x : x + 1] = odds[x, :1]
        yhi[x : x + 1] = odds[x, HY - 1 :]
    zed[...] = packed
    sent[...] = jnp.broadcast_to(jnp.sum(summed, axis=0, keepdims=True), sent.shape)


def first_kernel(
    from_xlo, from_xhi, from_ylo, from_yhi, from_zlo, from_zhi, h, a_hbm, v_hbm, spin_in,
    spin, side, column, energy, fields, clock, odds, gain, xlo, xhi, ylo, yhi, zed, sent, a, v, arrived,
):
    copies = fetch([(a_hbm.at[0], a), (v_hbm.at[0], v)], arrived)
    for p in range(2):
        spin[p, 0, :HY] = from_xlo[p]
        spin[p, BX + 1, :HY] = from_xhi[p]
        side[p] = jnp.where(lane_of(BX) < HZ, from_yhi[p], from_ylo[p])
        column[p] = jnp.where(z_parts(p), from_zlo[p], from_zhi[p])
    of_field = jnp.zeros((HY, BZ), F32)
    for x in range(BX):
        of_field = of_field + spin[1, x + 1, :HY] * h[1, x]
    fields[0] = jnp.zeros((8, BZ), F32)
    fields[1] = eighth(of_field)
    energy[...] = jnp.zeros(energy.shape, F32)
    clock[...] = jnp.zeros(clock.shape, F32)
    for copy in copies:
        copy.wait()
    rates(0, spin, side, column, odds, gain, h, a, v, xlo, xhi, ylo, yhi, zed, sent)


def section_kernel(
    act, half, where, gathered, from_xlo, from_xhi, from_ylo, from_yhi, from_zlo, from_zhi, h, a_hbm, v_hbm,
    spin_in, side_in, column_in, energy_in, fields_in, clock_in, odds_in, gain_in,
    spin, side, column, energy, fields, clock, odds, gain, xlo, xhi, ylo, yhi, zed, sent, a, v, arrived,
):
    k = where[0]
    copies = fetch([(a_hbm.at[act], a), (v_hbm.at[k], v)], arrived)
    halo = (from_xlo, from_xhi, from_ylo, from_yhi, from_zlo, from_zhi)
    advance(k, 1 - act, half, gathered, halo, spin, side, column, odds, gain, h, energy, fields, clock)
    for copy in copies:
        copy.wait()
    rates(act, spin, side, column, odds, gain, h, a, v, xlo, xhi, ylo, yhi, zed, sent)


def last_kernel(
    half, gathered, h, odds, gain, spin_in, energy_in, fields_in, clock_in,
    spin, energy, fields, clock, sent,
):
    advance(SECTIONS, (SECTIONS - 1) % 2, half, gathered, None, spin, None, None, odds, gain, h, energy, fields, clock)
    row = jnp.zeros((1, BZ), F32)
    for k in range(SECTIONS):
        value = jnp.sum(jnp.sum(energy[k], axis=0, keepdims=True), axis=1, keepdims=True)
        row = jnp.where(lane_of(1) == k, value, row)
    sent[...] = jnp.broadcast_to(row, sent.shape)


def unpack_kernel(spin, out):
    low = lane_of() < HZ
    narrow = shuffle_matrix(True)
    for x in range(BX):
        even_site, odd_site = spin[0, x + 1, :HY], spin[1, x + 1, :HY]
        odd = odd_row(x)
        even_z, odd_z = jnp.where(odd, odd_site, even_site), jnp.where(odd, even_site, odd_site)
        lower = jnp.where(low, even_z, roll(odd_z, HZ))
        upper = jnp.where(low, roll(even_z, HZ), odd_z)
        out[x, :HY] = matmul(lower, narrow, True)
        out[x, HY:] = matmul(upper, narrow, True)


def history_kernel(sites, gathered, clock, out):
    row = jnp.sum(gathered[...], axis=0, keepdims=True) / sites
    out[0:1, :] = row[:, :SECTIONS]
    out[1:2, :] = clock[0:1, :SECTIONS]


def call(kernel, name, inputs, outputs, aliases=None, far=(), far_out=(), scratch=(), flops=1000000):
    held, away = pl.BlockSpec(memory_space=pltpu.VMEM), pl.BlockSpec(memory_space=pltpu.HBM)
    inputs = [pltpu.with_memory_space_constraint(x, pltpu.HBM) if i in far else x for i, x in enumerate(inputs)]
    scalar = pl.BlockSpec(memory_space=pltpu.SMEM)
    return pl.pallas_call(
        kernel,
        name=name,
        out_shape=[pltpu.HBM(shape, F32) if i in far_out else jax.ShapeDtypeStruct(shape, F32) for i, shape in enumerate(outputs)],
        in_specs=[away if i in far else scalar if x.shape == (1,) else held for i, x in enumerate(inputs)],
        out_specs=[away if i in far_out else held for i in range(len(outputs))],
        input_output_aliases=aliases or {},
        scratch_shapes=scratch,
        compiler_params=pltpu.CompilerParams(vmem_limit_bytes=24 * 1024 * 1024),
        cost_estimate=pl.CostEstimate(flops=flops, bytes_accessed=1000000, transcendentals=0),
    )(*inputs)


def swap(xlo, xhi, ylo, yhi, zlo, zhi):
    got = []
    for axis, low, high in (("gx", xlo, xhi), ("gy", ylo, yhi), ("gz", zlo, zhi)):
        count = lax.axis_size(axis)
        up = [(i, (i + 1) % count) for i in range(count)]
        got.append(lax.ppermute(high, axis, up))
        got.append(lax.ppermute(low, axis, [(b, a) for a, b in up]))
    return got


def spread(sent):
    return lax.all_to_all(sent, AXES, 0, 0, tiled=True)


def body(occupancy, site_field, attempt_rate, uniforms):
    devices = lax.axis_size(AXES)
    sites = float(BX * BY * BZ * devices)
    half = sites / 2.0
    tile = (HY, BZ)
    spin_shape = (2, BX + 2, PITCH, BZ)
    block = (BX, *tile)
    faces = [tile, tile, (BX, BZ), (BX, BZ), tile]
    state = [spin_shape, (2, BX, BZ), (2, *tile), (SECTIONS, 8, BZ), (2, 8, BZ), (8, BZ), block, block]
    sent_shape = (devices, BZ)
    dma = pltpu.SemaphoreType.DMA
    streams = [pltpu.VMEM(block, F32), pltpu.VMEM(block, F32), dma((2,))]
    spin, *sides = call(
        spins_kernel, "spins", (occupancy,), [spin_shape] + [(2, *face) for face in faces], far=(0,),
        scratch=[pltpu.VMEM((BX, BY, BZ), jnp.int32), dma((BX // CHUNK,))],
    )
    halo = swap(*sides, sides[-1])
    h, a, v = call(
        fields_kernel, "fields", (site_field, attempt_rate, uniforms), [(2, *block), (2, *block), (SECTIONS, *block)],
        far=(0, 1, 2), far_out=(1, 2),
        scratch=[
            pltpu.VMEM((BX, BY, BZ), F32), pltpu.VMEM((BX, BY, BZ), F32), pltpu.VMEM((SECTIONS, BX, BY, HZ), F32),
            pltpu.VMEM((2, *block), F32), pltpu.VMEM((SECTIONS, *block), F32),
            dma((2,)), dma((SECTIONS,)), dma((SECTIONS + 1,)),
        ],
    )
    carried = call(
        first_kernel, "section0", (*halo, h, a, v, spin), state + faces + [sent_shape], {9: 0}, far=(7, 8), scratch=streams,
    )

    def section(k, act, carried):
        *kept, xlo, xhi, ylo, yhi, zed, sent = carried
        gathered = spread(sent)
        halo = swap(xlo, xhi, ylo, yhi, zed, zed)
        return call(
            functools.partial(section_kernel, act, half), "odd" if act else "even",
            (jnp.full((1,), k, jnp.int32), gathered, *halo, h, a, v, *kept), state + faces + [sent_shape],
            {11 + i: i for i in range(len(state))}, far=(9, 10), scratch=streams,
        )

    def pair(i, carried):
        return section(2 * i + 2, 0, section(2 * i + 1, 1, carried))

    carried = lax.fori_loop(0, SECTIONS // 2 - 1, pair, carried)
    carried = section(SECTIONS - 1, 1, carried)
    spin, _, _, energy, fields, clock, odds, gain = carried[: len(state)]
    gathered = spread(carried[-1])
    spin, energy, fields, clock, sent = call(
        functools.partial(last_kernel, half), "last",
        (gathered, h, odds, gain, spin, energy, fields, clock),
        [spin_shape, state[3], state[4], state[5], sent_shape], {4: 0, 5: 1, 6: 2, 7: 3},
    )
    gathered = spread(sent)
    (final,) = call(unpack_kernel, "unpack", (spin,), [(BX, BY, BZ)])
    (history,) = call(
        functools.partial(history_kernel, sites), "history", (gathered, clock), [(2, SECTIONS)],
    )
    return final, history


def solution(mesh):
    return jax.shard_map(
        body,
        mesh=mesh,
        in_specs=(P(*AXES), P(*AXES), P(*AXES), P(None, *AXES)),
        out_specs=(P(*AXES), P()),
        check_vma=False,
    )
```

```python
import functools

import jax
import jax.numpy as jnp
from jax import lax
from jax.experimental import pallas as pl
from jax.experimental.pallas import tpu as pltpu
from jax.sharding import PartitionSpec as P


SECTIONS = 8
AXES = ("gx", "gy", "gz")
BX, BY, BZ = 16, 64, 128
HY, HZ = BY // 2, BZ // 2
UNROLL = 4
CHUNK = 4
PITCH = HY + 8
F32, BF16 = jnp.float32, jnp.bfloat16


def lane_of(rows=HY):
    return lax.broadcasted_iota(jnp.int32, (rows, BZ), 1)


def odd_row(shift, rows=HY):
    return (lax.broadcasted_iota(jnp.int32, (rows, BZ), 0) + shift) % 2 == 1


def roll(value, shift):
    shift = shift % BZ
    return value if shift == 0 else pltpu.roll(value, shift, 1)


def shuffle_matrix(transposed):
    major = lax.broadcasted_iota(jnp.int32, (BZ, BZ), 1 if transposed else 0)
    minor = lax.broadcasted_iota(jnp.int32, (BZ, BZ), 0 if transposed else 1)
    return (minor == major // 2 + HZ * (major % 2)).astype(F32)


def matmul(a, b, exact):
    precision = lax.Precision.HIGHEST if exact else lax.Precision.DEFAULT
    return jnp.dot(a, b, precision=precision, preferred_element_type=F32)


def face_column(plane, x, phase):
    ends = jnp.where(odd_row(x + phase), roll(plane, HZ + 1), plane)
    return roll(ends, x)


def fetch(pairs, arrived):
    copies = [pltpu.make_async_copy(source, target, arrived.at[i]) for i, (source, target) in enumerate(pairs)]
    for copy in copies:
        copy.start()
    return copies


def split_sites(mixed, odd, low):
    lower, upper = mixed[:HY], mixed[HY:]
    lower_turned, upper_turned = roll(lower, HZ), roll(upper, HZ)
    even_site = jnp.where(low, jnp.where(odd, lower_turned, lower), jnp.where(odd, upper, upper_turned))
    odd_site = jnp.where(low, jnp.where(odd, lower, lower_turned), jnp.where(odd, upper_turned, upper))
    return even_site, odd_site


def spins_kernel(occ_hbm, spin, xlo, xhi, ylo, yhi, zed, occ, arrived):
    copies = fetch([(occ_hbm.at[pl.ds(c * CHUNK, CHUNK)], occ.at[pl.ds(c * CHUNK, CHUNK)]) for c in range(BX // CHUNK)], arrived)
    lane = lane_of()
    wide = shuffle_matrix(False)
    columns = [jnp.zeros((HY, BZ), F32)] * 2
    for x in range(BX):
        if x % CHUNK == 0:
            copies[x // CHUNK].wait()
        planes = split_sites(matmul(2.0 * occ[x].astype(F32) - 1.0, wide, False), odd_row(x), lane < HZ)
        for p, plane in enumerate(planes):
            spin[p, x + 1, :HY] = plane
            ylo[p, x : x + 1] = plane[:1]
            yhi[p, x : x + 1] = plane[HY - 1 :]
            columns[p] = jnp.where(lane % HZ == x, face_column(plane, x, p), columns[p])
            if x == 0:
                xlo[p] = plane
            if x == BX - 1:
                xhi[p] = plane
    for p in range(2):
        zed[p] = columns[p]


def shuffled(value, wide):
    high = value.astype(BF16)
    rest = value - high.astype(F32)
    middle = rest.astype(BF16)
    low = (rest - middle.astype(F32)).astype(BF16)
    rows = value.shape[0]
    parts = jnp.dot(jnp.concatenate([high, middle, low], axis=0), wide, preferred_element_type=F32)
    return parts[:rows] + parts[rows : 2 * rows] + parts[2 * rows :]


def fields_kernel(
    field_hbm, attempt_hbm, uniforms, h, a, v0, v_out, field, attempt, raw, inverse, v, arrived, drawn, left,
):
    copies = fetch([(field_hbm, field), (attempt_hbm, attempt)], arrived)
    draws = fetch([(uniforms.at[k], raw.at[k]) for k in range(SECTIONS)], drawn)
    low = lane_of() < HZ
    wide = shuffle_matrix(False).astype(BF16)
    for copy in copies:
        copy.wait()

    @pl.loop(0, BX // UNROLL)
    def _(i):
        for j in range(UNROLL):
            x = i * UNROLL + j
            h[0, x], h[1, x] = split_sites(shuffled(field[x], wide), odd_row(j), low)
            even_site, odd_site = split_sites(shuffled(attempt[x], wide), odd_row(j), low)
            a[0, x], a[1, x] = even_site, odd_site
            inverse[0, x], inverse[1, x] = 1.0 / even_site, 1.0 / odd_site

    writes = []
    for k in range(SECTIONS):
        draws[k].wait()

        @pl.loop(0, BX // UNROLL)
        def _(i):
            for j in range(UNROLL):
                x = i * UNROLL + j
                scaled = jnp.concatenate([raw[k, x, :HY], raw[k, x, HY:]], axis=1) * inverse[k % 2, x]
                if k == 0:
                    v0[x] = scaled
                else:
                    v[k, x] = scaled

        if k > 0:
            write = pltpu.make_async_copy(v.at[k], v_out.at[k], left.at[k])
            write.start()
            writes.append(write)
    for write in writes:
        write.wait()


def z_parts(phase):
    lane = lane_of()
    row = lax.broadcasted_iota(jnp.int32, (HY, BZ), 0)
    return (lane % HZ + row + phase) % 2 == 1


def flip_of(total, half):
    ratio = total / half
    square = ratio * ratio
    return lambda odds: 1.0 - 2.0 / (1.0 + odds * square)


def eighth(value):
    return value[0:8] + value[8:16] + value[16:24] + value[24:32]


def advance(k, p, half, gathered, halo, spin, side, column, odds, gain, h, energy, fields, clock):
    total = jnp.sum(jnp.sum(gathered[...], axis=0, keepdims=True), axis=1, keepdims=True)
    flip = flip_of(total, half)
    elapsed = clock[1:2, :] + half / total
    clock[1:2, :] = elapsed
    clock[0:1, :] = jnp.where(lane_of(1) == k - 1, elapsed, clock[0:1, :])
    of_gain = jnp.zeros((HY, BZ), F32)
    of_field = jnp.zeros((HY, BZ), F32)

    def step(i, carry):
        of_gain, of_field = carry
        for j in range(UNROLL):
            x = i * UNROLL + j
            new = spin[p, x + 1, :HY] * flip(odds[x])
            spin[p, x + 1, :HY] = new
            of_gain = of_gain + new * gain[x]
            of_field = of_field + new * h[p, x]
        return of_gain, of_field

    of_gain, of_field = lax.fori_loop(0, BX // UNROLL, step, (of_gain, of_field))
    fields[p] = eighth(of_field)
    energy[k - 1] = -eighth(of_gain) - fields[1 - p]
    if halo is None:
        return
    from_xlo, from_xhi, from_ylo, from_yhi, from_zlo, from_zhi = halo
    spin[p, 0, :HY] = spin[p, 0, :HY] * flip(from_xlo[...])
    spin[p, BX + 1, :HY] = spin[p, BX + 1, :HY] * flip(from_xhi[...])
    side[p] = side[p] * flip(jnp.where(lane_of(BX) < HZ, from_yhi[...], from_ylo[...]))
    column[p] = column[p] * flip(jnp.where(z_parts(p), from_zlo[...], from_zhi[...]))


def rates(act, spin, side, column, odds, gain, h, a, v, xlo, xhi, ylo, yhi, zed, sent):
    p = 1 - act
    lane = lane_of()
    one_row = lane_of(1)
    for x in range(BX):
        first, last = spin[p, x + 1, :1], spin[p, x + 1, HY - 1 : HY]
        beyond = side[p, x : x + 1]
        spin[p, x + 1, HY + 1 : HY + 2] = roll(jnp.where(one_row < HZ, last, beyond), HZ)
        spin[p, x + 1, HY : HY + 1] = roll(jnp.where(one_row < HZ, beyond, first), HZ)
    ends = column[p]
    top = lax.broadcasted_iota(jnp.int32, (HY, BZ), 0) == 0

    def step(i, carry):
        packed, summed = carry
        for j in range(UNROLL):
            x = i * UNROLL + j
            odd = odd_row(j + act)
            here = spin[p, x + 1, :HY]
            turned = jnp.where(odd, roll(here, -1), roll(here, 1))
            edge = jnp.where(odd, pltpu.roll(ends, (HZ - 1 - x) % BZ, 1), pltpu.roll(ends, (BZ - x) % BZ, 1))
            at_edge = lane % HZ == jnp.where(odd, HZ - 1, 0)
            beside = spin[p, x, :HY] + spin[p, x + 2, :HY]
            beside = beside + jnp.where(top, spin[p, x + 1, HY + 1 : HY + 2], pltpu.roll(here, 1, 0)) + spin[p, x + 1, 1 : HY + 1]
            beside = beside + here + jnp.where(at_edge, edge, turned)
            g = h[act, x] - 0.5 * beside
            gain[x] = g
            grown = 1.0 + jnp.exp(2.0 * spin[act, x + 1, :HY] * g)
            summed = summed + a[act, x] / grown
            root = v[x] * grown
            square = root * root
            odds[x] = square
            marked = jnp.where(odd, roll(square, HZ + 1), square)
            packed = jnp.where(lane % HZ == x, pltpu.roll(marked, x, 1), packed)
        return packed, summed

    packed, summed = lax.fori_loop(0, BX // UNROLL, step, (jnp.zeros((HY, BZ), F32), jnp.zeros((HY, BZ), F32)))
    xlo[...] = odds[0]
    xhi[...] = odds[BX - 1]
    for x in range(BX):
        ylo[x : x + 1] = odds[x, :1]
        yhi[x : x + 1] = odds[x, HY - 1 :]
    zed[...] = packed
    sent[...] = jnp.broadcast_to(jnp.sum(summed, axis=0, keepdims=True), sent.shape)


def first_kernel(
    from_xlo, from_xhi, from_ylo, from_yhi, from_zlo, from_zhi, h, a, v, v_hbm, spin_in,
    spin, side, column, energy, fields, clock, odds, gain, xlo, xhi, ylo, yhi, zed, sent, v_next, arrived,
):
    copies = fetch([(v_hbm.at[1], v_next)], arrived)
    for p in range(2):
        spin[p, 0, :HY] = from_xlo[p]
        spin[p, BX + 1, :HY] = from_xhi[p]
        side[p] = jnp.where(lane_of(BX) < HZ, from_yhi[p], from_ylo[p])
        column[p] = jnp.where(z_parts(p), from_zlo[p], from_zhi[p])
    of_field = jnp.zeros((HY, BZ), F32)
    for x in range(BX):
        of_field = of_field + spin[1, x + 1, :HY] * h[1, x]
    fields[0] = jnp.zeros((8, BZ), F32)
    fields[1] = eighth(of_field)
    energy[...] = jnp.zeros(energy.shape, F32)
    clock[...] = jnp.zeros(clock.shape, F32)
    rates(0, spin, side, column, odds, gain, h, a, v, xlo, xhi, ylo, yhi, zed, sent)
    copies[0].wait()


def section_kernel(
    act, half, where, gathered, from_xlo, from_xhi, from_ylo, from_yhi, from_zlo, from_zhi, h, a, v, v_hbm,
    spin_in, side_in, column_in, energy_in, fields_in, clock_in, odds_in, gain_in,
    spin, side, column, energy, fields, clock, odds, gain, xlo, xhi, ylo, yhi, zed, sent, v_next, arrived,
):
    k = where[0]
    copies = fetch([(v_hbm.at[jnp.minimum(k + 1, SECTIONS - 1)], v_next)], arrived)
    halo = (from_xlo, from_xhi, from_ylo, from_yhi, from_zlo, from_zhi)
    advance(k, 1 - act, half, gathered, halo, spin, side, column, odds, gain, h, energy, fields, clock)
    rates(act, spin, side, column, odds, gain, h, a, v, xlo, xhi, ylo, yhi, zed, sent)
    copies[0].wait()


def last_kernel(
    half, gathered, h, odds, gain, spin_in, energy_in, fields_in, clock_in,
    spin, energy, fields, clock, sent,
):
    advance(SECTIONS, (SECTIONS - 1) % 2, half, gathered, None, spin, None, None, odds, gain, h, energy, fields, clock)
    row = jnp.zeros((1, BZ), F32)
    for k in range(SECTIONS):
        value = jnp.sum(jnp.sum(energy[k], axis=0, keepdims=True), axis=1, keepdims=True)
        row = jnp.where(lane_of(1) == k, value, row)
    sent[...] = jnp.broadcast_to(row, sent.shape)


def unpack_kernel(spin, out):
    low = lane_of() < HZ
    narrow = shuffle_matrix(True)
    for x in range(BX):
        even_site, odd_site = spin[0, x + 1, :HY], spin[1, x + 1, :HY]
        odd = odd_row(x)
        even_z, odd_z = jnp.where(odd, odd_site, even_site), jnp.where(odd, even_site, odd_site)
        lower = jnp.where(low, even_z, roll(odd_z, HZ))
        upper = jnp.where(low, roll(even_z, HZ), odd_z)
        out[x, :HY] = matmul(lower, narrow, True)
        out[x, HY:] = matmul(upper, narrow, True)


def history_kernel(sites, gathered, clock, out):
    row = jnp.sum(gathered[...], axis=0, keepdims=True) / sites
    out[0:1, :] = row[:, :SECTIONS]
    out[1:2, :] = clock[0:1, :SECTIONS]


def call(kernel, inputs, outputs, aliases=None, far=(), far_out=(), scratch=(), flops=1000000):
    held, away = pl.BlockSpec(memory_space=pltpu.VMEM), pl.BlockSpec(memory_space=pltpu.HBM)
    inputs = [pltpu.with_memory_space_constraint(x, pltpu.HBM) if i in far else x for i, x in enumerate(inputs)]
    scalar = pl.BlockSpec(memory_space=pltpu.SMEM)
    return pl.pallas_call(
        kernel,
        out_shape=[pltpu.HBM(shape, F32) if i in far_out else jax.ShapeDtypeStruct(shape, F32) for i, shape in enumerate(outputs)],
        in_specs=[away if i in far else scalar if x.shape == (1,) else held for i, x in enumerate(inputs)],
        out_specs=[away if i in far_out else held for i in range(len(outputs))],
        input_output_aliases=aliases or {},
        scratch_shapes=scratch,
        compiler_params=pltpu.CompilerParams(vmem_limit_bytes=24 * 1024 * 1024),
        cost_estimate=pl.CostEstimate(flops=flops, bytes_accessed=1000000, transcendentals=0),
    )(*inputs)


def swap(xlo, xhi, ylo, yhi, zlo, zhi):
    got = []
    for axis, low, high in (("gx", xlo, xhi), ("gy", ylo, yhi), ("gz", zlo, zhi)):
        count = lax.axis_size(axis)
        up = [(i, (i + 1) % count) for i in range(count)]
        got.append(lax.ppermute(high, axis, up))
        got.append(lax.ppermute(low, axis, [(b, a) for a, b in up]))
    return got


def spread(sent):
    return lax.all_to_all(sent, AXES, 0, 0, tiled=True)


def body(occupancy, site_field, attempt_rate, uniforms):
    devices = lax.axis_size(AXES)
    sites = float(BX * BY * BZ * devices)
    half = sites / 2.0
    tile = (HY, BZ)
    spin_shape = (2, BX + 2, PITCH, BZ)
    block = (BX, *tile)
    faces = [tile, tile, (BX, BZ), (BX, BZ), tile]
    state = [spin_shape, (2, BX, BZ), (2, *tile), (SECTIONS, 8, BZ), (2, 8, BZ), (8, BZ), block, block]
    sent_shape = (devices, BZ)
    dma = pltpu.SemaphoreType.DMA
    streams = [dma((1,))]
    spin, *sides = call(
        spins_kernel, (occupancy,), [spin_shape] + [(2, *face) for face in faces], far=(0,),
        scratch=[pltpu.VMEM((BX, BY, BZ), jnp.int32), dma((BX // CHUNK,))],
    )
    halo = swap(*sides, sides[-1])
    h, a, v, draws = call(
        fields_kernel, (site_field, attempt_rate, uniforms), [(2, *block), (2, *block), block, (SECTIONS, *block)],
        far=(0, 1, 2), far_out=(3,),
        scratch=[
            pltpu.VMEM((BX, BY, BZ), F32), pltpu.VMEM((BX, BY, BZ), F32), pltpu.VMEM((SECTIONS, BX, BY, HZ), F32),
            pltpu.VMEM((2, *block), F32), pltpu.VMEM((SECTIONS, *block), F32),
            dma((2,)), dma((SECTIONS,)), dma((SECTIONS,)),
        ],
    )
    carried = call(
        first_kernel, (*halo, h, a, v, draws, spin), state + faces + [sent_shape, block], {10: 0}, far=(9,), scratch=streams,
    )

    def section(k, act, carried):
        *kept, xlo, xhi, ylo, yhi, zed, sent, v = carried
        gathered = spread(sent)
        halo = swap(xlo, xhi, ylo, yhi, zed, zed)
        return call(
            functools.partial(section_kernel, act, half),
            (jnp.full((1,), k, jnp.int32), gathered, *halo, h, a, v, draws, *kept), state + faces + [sent_shape, block],
            {12 + i: i for i in range(len(state))}, far=(11,), scratch=streams,
        )

    def pair(i, carried):
        return section(2 * i + 2, 0, section(2 * i + 1, 1, carried))

    carried = lax.fori_loop(0, SECTIONS // 2 - 1, pair, carried)
    carried = section(SECTIONS - 1, 1, carried)
    spin, _, _, energy, fields, clock, odds, gain = carried[: len(state)]
    gathered = spread(carried[-2])
    spin, energy, fields, clock, sent = call(
        functools.partial(last_kernel, half),
        (gathered, h, odds, gain, spin, energy, fields, clock),
        [spin_shape, state[3], state[4], state[5], sent_shape], {4: 0, 5: 1, 6: 2, 7: 3},
    )
    gathered = spread(sent)
    (final,) = call(unpack_kernel, (spin,), [(BX, BY, BZ)])
    (history,) = call(functools.partial(history_kernel, sites), (gathered, clock), [(2, SECTIONS)])
    return final, history


def solution(mesh):
    return jax.shard_map(
        body,
        mesh=mesh,
        in_specs=(P(*AXES), P(*AXES), P(*AXES), P(None, *AXES)),
        out_specs=(P(*AXES), P()),
        check_vma=False,
    )
```

```python
import functools

import jax
import jax.numpy as jnp
from jax import lax
from jax.experimental import pallas as pl
from jax.experimental.pallas import tpu as pltpu
from jax.sharding import PartitionSpec as P


SECTIONS = 8
AXES = ("gx", "gy", "gz")
BX, BY, BZ = 16, 64, 128
HY, HZ = BY // 2, BZ // 2
UNROLL = 4
CHUNK = 4
PITCH = HY + 8
F32, BF16 = jnp.float32, jnp.bfloat16


def lane_of(rows=HY):
    return lax.broadcasted_iota(jnp.int32, (rows, BZ), 1)


def odd_row(shift, rows=HY):
    return (lax.broadcasted_iota(jnp.int32, (rows, BZ), 0) + shift) % 2 == 1


def roll(value, shift):
    shift = shift % BZ
    return value if shift == 0 else pltpu.roll(value, shift, 1)


def shuffle_matrix(transposed):
    major = lax.broadcasted_iota(jnp.int32, (BZ, BZ), 1 if transposed else 0)
    minor = lax.broadcasted_iota(jnp.int32, (BZ, BZ), 0 if transposed else 1)
    return (minor == major // 2 + HZ * (major % 2)).astype(F32)


def matmul(a, b, exact):
    precision = lax.Precision.HIGHEST if exact else lax.Precision.DEFAULT
    return jnp.dot(a, b, precision=precision, preferred_element_type=F32)


def add_face(column, plane, x, odd):
    slot = (2 * x - jnp.where(odd, 1, 0)) % HZ
    return jnp.where(lane_of() % HZ == slot, pltpu.roll(plane, 2 * x, 1), column)


def fetch(pairs, arrived):
    copies = [pltpu.make_async_copy(source, target, arrived.at[i]) for i, (source, target) in enumerate(pairs)]
    for copy in copies:
        copy.start()
    return copies


def split_sites(mixed, odd, low):
    lower, upper = mixed[:HY], mixed[HY:]
    lower_turned, upper_turned = roll(lower, HZ), roll(upper, HZ)
    even_site = jnp.where(low, jnp.where(odd, lower_turned, lower), jnp.where(odd, upper, upper_turned))
    odd_site = jnp.where(low, jnp.where(odd, lower, lower_turned), jnp.where(odd, upper_turned, upper))
    return even_site, odd_site


def spins_kernel(where, occ_hbm, spin, x_one, x_two, y_one, y_two, zed, occ, arrived):
    copies = fetch([(occ_hbm.at[pl.ds(c * CHUNK, CHUNK)], occ.at[pl.ds(c * CHUNK, CHUNK)]) for c in range(BX // CHUNK)], arrived)
    lane = lane_of()
    wide = shuffle_matrix(False)
    columns = [jnp.zeros((HY, BZ), F32)] * 2
    for x in range(BX):
        if x % CHUNK == 0:
            copies[x // CHUNK].wait()
        planes = split_sites(matmul(2.0 * occ[x].astype(F32) - 1.0, wide, False), odd_row(x), lane < HZ)
        for p, plane in enumerate(planes):
            spin[p, x + 1, :HY] = plane
            y_one[p, x : x + 1], y_two[p, x : x + 1] = sort_faces(where[2], plane[:1], plane[HY - 1 :])
            columns[p] = add_face(columns[p], plane, x, odd_row(x + p))
    for p in range(2):
        x_one[p], x_two[p] = sort_faces(where[1], spin[p, 1, :HY], spin[p, BX, :HY])
        zed[p] = columns[p]


def shuffled(value, wide):
    high = value.astype(BF16)
    rest = value - high.astype(F32)
    middle = rest.astype(BF16)
    low = (rest - middle.astype(F32)).astype(BF16)
    rows = value.shape[0]
    parts = jnp.dot(jnp.concatenate([high, middle, low], axis=0), wide, preferred_element_type=F32)
    return parts[:rows] + parts[rows : 2 * rows] + parts[2 * rows :]


def fields_kernel(
    field_hbm, attempt_hbm, uniforms, h, a, v0, v_out, field, attempt, raw, inverse, v, arrived, drawn, left,
):
    copies = fetch([(field_hbm, field), (attempt_hbm, attempt)], arrived)
    draws = fetch([(uniforms.at[k], raw.at[k]) for k in range(SECTIONS)], drawn)
    low = lane_of() < HZ
    wide = shuffle_matrix(False).astype(BF16)
    for copy in copies:
        copy.wait()

    @pl.loop(0, BX // UNROLL)
    def _(i):
        for j in range(UNROLL):
            x = i * UNROLL + j
            h[0, x], h[1, x] = split_sites(shuffled(field[x], wide), odd_row(j), low)
            even_site, odd_site = split_sites(shuffled(attempt[x], wide), odd_row(j), low)
            a[0, x], a[1, x] = even_site, odd_site
            inverse[0, x], inverse[1, x] = 1.0 / even_site, 1.0 / odd_site

    writes = []
    for k in range(SECTIONS):
        draws[k].wait()

        @pl.loop(0, BX // UNROLL)
        def _(i):
            for j in range(UNROLL):
                x = i * UNROLL + j
                scaled = jnp.concatenate([raw[k, x, :HY], raw[k, x, HY:]], axis=1) * inverse[k % 2, x]
                if k == 0:
                    v0[x] = scaled
                else:
                    v[k, x] = scaled

        if k > 0:
            write = pltpu.make_async_copy(v.at[k], v_out.at[k], left.at[k])
            write.start()
            writes.append(write)
    for write in writes:
        write.wait()


def sort_halo(even, first, second):
    even = even == 1
    return jnp.where(even, second, first), jnp.where(even, first, second)


def sort_faces(where, low, high):
    even = where == 1
    return jnp.where(even, high, low), jnp.where(even, low, high)


def halo_parts(where, x_one, x_two, y_one, y_two, z_one, z_two):
    low_x, high_x = sort_halo(where[1], x_one, x_two)
    low_y, high_y = sort_halo(where[2], y_one, y_two)
    low_z, high_z = sort_halo(where[3], z_one, z_two)
    return low_x, high_x, jnp.where(lane_of(BX) < HZ, high_y, low_y), jnp.where(lane_of() % 2 == 1, low_z, high_z)


def flip_of(total, half):
    ratio = total / half
    square = ratio * ratio
    return lambda odds: 1.0 - 2.0 / (1.0 + odds * square)


def eighth(value):
    return value[0:8] + value[8:16] + value[16:24] + value[24:32]


def advance(k, p, half, gathered, halo, spin, side, column, odds, gain, h, energy, fields, clock):
    total = jnp.sum(jnp.sum(gathered[...], axis=0, keepdims=True), axis=1, keepdims=True)
    flip = flip_of(total, half)
    elapsed = clock[1:2, :] + half / total
    clock[1:2, :] = elapsed
    clock[0:1, :] = jnp.where(lane_of(1) == k - 1, elapsed, clock[0:1, :])
    of_gain = jnp.zeros((HY, BZ), F32)
    of_field = jnp.zeros((HY, BZ), F32)

    def step(i, carry):
        of_gain, of_field = carry
        for j in range(UNROLL):
            x = i * UNROLL + j
            new = spin[p, x + 1, :HY] * flip(odds[x])
            spin[p, x + 1, :HY] = new
            of_gain = of_gain + new * gain[x]
            of_field = of_field + new * h[p, x]
        return of_gain, of_field

    of_gain, of_field = lax.fori_loop(0, BX // UNROLL, step, (of_gain, of_field))
    fields[p] = eighth(of_field)
    energy[k - 1] = -eighth(of_gain) - fields[1 - p]
    if halo is None:
        return
    low_x, high_x, y_side, z_side = halo
    spin[p, 0, :HY] = spin[p, 0, :HY] * flip(low_x)
    spin[p, BX + 1, :HY] = spin[p, BX + 1, :HY] * flip(high_x)
    side[p] = side[p] * flip(y_side)
    column[p] = column[p] * flip(z_side)


def rates(act, where, spin, side, column, odds, gain, h, a, v, x_one, x_two, y_one, y_two, zed, sent):
    p = 1 - act
    lane = lane_of()
    one_row = lane_of(1)
    for x in range(BX):
        first, last = spin[p, x + 1, :1], spin[p, x + 1, HY - 1 : HY]
        beyond = side[p, x : x + 1]
        spin[p, x + 1, HY + 1 : HY + 2] = roll(jnp.where(one_row < HZ, last, beyond), HZ)
        spin[p, x + 1, HY : HY + 1] = roll(jnp.where(one_row < HZ, beyond, first), HZ)
    ends = column[p]
    top = lax.broadcasted_iota(jnp.int32, (HY, BZ), 0) == 0

    def step(i, carry):
        packed, summed = carry
        for j in range(UNROLL):
            x = i * UNROLL + j
            odd = odd_row(j + act)
            here = spin[p, x + 1, :HY]
            joined = jnp.where(lane % HZ == jnp.where(odd, 0, HZ - 1), pltpu.roll(ends, (BZ + HZ - 2 * x) % BZ, 1), here)
            turned = jnp.where(odd, roll(joined, -1), roll(joined, 1))
            beside = spin[p, x, :HY] + spin[p, x + 2, :HY]
            beside = beside + jnp.where(top, spin[p, x + 1, HY + 1 : HY + 2], pltpu.roll(here, 1, 0)) + spin[p, x + 1, 1 : HY + 1]
            beside = beside + here + turned
            g = h[act, x] - 0.5 * beside
            gain[x] = g
            grown = 1.0 + jnp.exp(2.0 * spin[act, x + 1, :HY] * g)
            summed = summed + a[act, x] / grown
            root = v[x] * grown
            square = root * root
            odds[x] = square
            packed = add_face(packed, square, x, odd)
        return packed, summed

    packed, summed = lax.fori_loop(0, BX // UNROLL, step, (jnp.zeros((HY, BZ), F32), jnp.zeros((HY, BZ), F32)))
    x_one[...], x_two[...] = sort_faces(where[1], odds[0], odds[BX - 1])
    for x in range(BX):
        y_one[x : x + 1], y_two[x : x + 1] = sort_faces(where[2], odds[x, :1], odds[x, HY - 1 :])
    zed[...] = packed
    sent[...] = jnp.broadcast_to(jnp.sum(summed, axis=0, keepdims=True), sent.shape)


def first_kernel(
    where, from_x_one, from_x_two, from_y_one, from_y_two, from_z_one, from_z_two, h, a, v, v_hbm, spin_in,
    spin, side, column, energy, fields, clock, odds, gain, x_one, x_two, y_one, y_two, zed, sent, v_next, arrived,
):
    copies = fetch([(v_hbm.at[1], v_next)], arrived)
    for p in range(2):
        spin[p, 0, :HY], spin[p, BX + 1, :HY], side[p], column[p] = halo_parts(
            where, from_x_one[p], from_x_two[p], from_y_one[p], from_y_two[p], from_z_one[p], from_z_two[p]
        )
    of_field = jnp.zeros((HY, BZ), F32)
    for x in range(BX):
        of_field = of_field + spin[1, x + 1, :HY] * h[1, x]
    fields[0] = jnp.zeros((8, BZ), F32)
    fields[1] = eighth(of_field)
    energy[...] = jnp.zeros(energy.shape, F32)
    clock[...] = jnp.zeros(clock.shape, F32)
    rates(0, where, spin, side, column, odds, gain, h, a, v, x_one, x_two, y_one, y_two, zed, sent)
    copies[0].wait()


def section_kernel(
    act, half, where, gathered, from_x_one, from_x_two, from_y_one, from_y_two, from_z_one, from_z_two, h, a, v, v_hbm,
    spin_in, side_in, column_in, energy_in, fields_in, clock_in, odds_in, gain_in,
    spin, side, column, energy, fields, clock, odds, gain, x_one, x_two, y_one, y_two, zed, sent, v_next, arrived,
):
    k = where[0]
    copies = fetch([(v_hbm.at[jnp.minimum(k + 1, SECTIONS - 1)], v_next)], arrived)
    halo = halo_parts(
        where, from_x_one[...], from_x_two[...], from_y_one[...], from_y_two[...], from_z_one[...], from_z_two[...]
    )
    advance(k, 1 - act, half, gathered, halo, spin, side, column, odds, gain, h, energy, fields, clock)
    rates(act, where, spin, side, column, odds, gain, h, a, v, x_one, x_two, y_one, y_two, zed, sent)
    copies[0].wait()


def last_kernel(
    half, gathered, h, odds, gain, spin_in, energy_in, fields_in, clock_in,
    spin, energy, fields, clock, sent,
):
    advance(SECTIONS, (SECTIONS - 1) % 2, half, gathered, None, spin, None, None, odds, gain, h, energy, fields, clock)
    row = jnp.zeros((1, BZ), F32)
    for k in range(SECTIONS):
        value = jnp.sum(jnp.sum(energy[k], axis=0, keepdims=True), axis=1, keepdims=True)
        row = jnp.where(lane_of(1) == k, value, row)
    sent[...] = jnp.broadcast_to(row, sent.shape)


def unpack_kernel(spin, out):
    low = lane_of() < HZ
    narrow = shuffle_matrix(True)
    for x in range(BX):
        even_site, odd_site = spin[0, x + 1, :HY], spin[1, x + 1, :HY]
        odd = odd_row(x)
        even_z, odd_z = jnp.where(odd, odd_site, even_site), jnp.where(odd, even_site, odd_site)
        lower = jnp.where(low, even_z, roll(odd_z, HZ))
        upper = jnp.where(low, roll(even_z, HZ), odd_z)
        out[x, :HY] = matmul(lower, narrow, True)
        out[x, HY:] = matmul(upper, narrow, True)


def history_kernel(sites, gathered, clock, out):
    row = jnp.sum(gathered[...], axis=0, keepdims=True) / sites
    out[0:1, :] = row[:, :SECTIONS]
    out[1:2, :] = clock[0:1, :SECTIONS]


def call(kernel, inputs, outputs, aliases=None, far=(), far_out=(), scratch=(), flops=1000000):
    held, away = pl.BlockSpec(memory_space=pltpu.VMEM), pl.BlockSpec(memory_space=pltpu.HBM)
    inputs = [pltpu.with_memory_space_constraint(x, pltpu.HBM) if i in far else x for i, x in enumerate(inputs)]
    scalar = pl.BlockSpec(memory_space=pltpu.SMEM)
    return pl.pallas_call(
        kernel,
        out_shape=[pltpu.HBM(shape, F32) if i in far_out else jax.ShapeDtypeStruct(shape, F32) for i, shape in enumerate(outputs)],
        in_specs=[away if i in far else scalar if x.shape == (4,) else held for i, x in enumerate(inputs)],
        out_specs=[away if i in far_out else held for i in range(len(outputs))],
        input_output_aliases=aliases or {},
        scratch_shapes=scratch,
        compiler_params=pltpu.CompilerParams(vmem_limit_bytes=24 * 1024 * 1024),
        cost_estimate=pl.CostEstimate(flops=flops, bytes_accessed=1000000, transcendentals=0),
    )(*inputs)


def swap(x_one, x_two, y_one, y_two, z_one, z_two):
    got = []
    for axis, one, two in (("gx", x_one, x_two), ("gy", y_one, y_two), ("gz", z_one, z_two)):
        count = lax.axis_size(axis)
        for block, shift in ((one, 0), (two, 1)):
            pairs = [(i, (i + (1 if i % 2 == shift else -1)) % count) for i in range(count)]
            got.append(lax.ppermute(block, axis, pairs))
    return got


def spread(sent):
    return lax.all_to_all(sent, AXES, 0, 0, tiled=True)


def body(occupancy, site_field, attempt_rate, uniforms):
    devices = lax.axis_size(AXES)
    sites = float(BX * BY * BZ * devices)
    half = sites / 2.0
    tile = (HY, BZ)
    spin_shape = (2, BX + 2, PITCH, BZ)
    block = (BX, *tile)
    faces = [tile, tile, (BX, BZ), (BX, BZ), tile]
    state = [spin_shape, (2, BX, BZ), (2, *tile), (SECTIONS, 8, BZ), (2, 8, BZ), (8, BZ), block, block]
    sent_shape = (devices, BZ)
    dma = pltpu.SemaphoreType.DMA
    evens = [1 - lax.axis_index(axis) % 2 for axis in AXES]

    def where(k):
        return jnp.stack([jnp.asarray(k, jnp.int32), *evens]).astype(jnp.int32)

    streams = [dma((1,))]
    spin, *sides = call(
        spins_kernel, (where(0), occupancy), [spin_shape] + [(2, *face) for face in faces], far=(1,),
        scratch=[pltpu.VMEM((BX, BY, BZ), jnp.int32), dma((BX // CHUNK,))],
    )
    halo = swap(*sides, sides[-1])
    h, a, v, draws = call(
        fields_kernel, (site_field, attempt_rate, uniforms), [(2, *block), (2, *block), block, (SECTIONS, *block)],
        far=(0, 1, 2), far_out=(3,),
        scratch=[
            pltpu.VMEM((BX, BY, BZ), F32), pltpu.VMEM((BX, BY, BZ), F32), pltpu.VMEM((SECTIONS, BX, BY, HZ), F32),
            pltpu.VMEM((2, *block), F32), pltpu.VMEM((SECTIONS, *block), F32),
            dma((2,)), dma((SECTIONS,)), dma((SECTIONS,)),
        ],
    )
    carried = call(
        first_kernel, (where(0), *halo, h, a, v, draws, spin), state + faces + [sent_shape, block], {11: 0}, far=(10,), scratch=streams,
    )

    def section(k, act, carried):
        *kept, x_one, x_two, y_one, y_two, zed, sent, v = carried
        gathered = spread(sent)
        halo = swap(x_one, x_two, y_one, y_two, zed, zed)
        return call(
            functools.partial(section_kernel, act, half),
            (where(k), gathered, *halo, h, a, v, draws, *kept), state + faces + [sent_shape, block],
            {12 + i: i for i in range(len(state))}, far=(11,), scratch=streams,
        )

    def pair(i, carried):
        return section(2 * i + 2, 0, section(2 * i + 1, 1, carried))

    carried = lax.fori_loop(0, SECTIONS // 2 - 1, pair, carried)
    carried = section(SECTIONS - 1, 1, carried)
    spin, _, _, energy, fields, clock, odds, gain = carried[: len(state)]
    gathered = spread(carried[-2])
    spin, energy, fields, clock, sent = call(
        functools.partial(last_kernel, half),
        (gathered, h, odds, gain, spin, energy, fields, clock),
        [spin_shape, state[3], state[4], state[5], sent_shape], {4: 0, 5: 1, 6: 2, 7: 3},
    )
    gathered = spread(sent)
    (final,) = call(unpack_kernel, (spin,), [(BX, BY, BZ)])
    (history,) = call(functools.partial(history_kernel, sites), (gathered, clock), [(2, SECTIONS)])
    return final, history


def solution(mesh):
    return jax.shard_map(
        body,
        mesh=mesh,
        in_specs=(P(*AXES), P(*AXES), P(*AXES), P(None, *AXES)),
        out_specs=(P(*AXES), P()),
        check_vma=False,
    )
```

```python
import functools

import jax
import jax.numpy as jnp
from jax import lax
from jax.experimental import pallas as pl
from jax.experimental.pallas import tpu as pltpu
from jax.sharding import PartitionSpec as P


SECTIONS = 8
AXES = ("gx", "gy", "gz")
BX, BY, BZ = 16, 64, 128
HY, HZ = BY // 2, BZ // 2
UNROLL = 16
CHUNK = 4
PITCH = HY + 8
F32, BF16 = jnp.float32, jnp.bfloat16


def lane_of(rows=HY):
    return lax.broadcasted_iota(jnp.int32, (rows, BZ), 1)


def odd_row(shift, rows=HY):
    return (lax.broadcasted_iota(jnp.int32, (rows, BZ), 0) + shift) % 2 == 1


def roll(value, shift):
    shift = shift % BZ
    return value if shift == 0 else pltpu.roll(value, shift, 1)


def shuffle_matrix(transposed):
    major = lax.broadcasted_iota(jnp.int32, (BZ, BZ), 1 if transposed else 0)
    minor = lax.broadcasted_iota(jnp.int32, (BZ, BZ), 0 if transposed else 1)
    return (minor == major // 2 + HZ * (major % 2)).astype(F32)


def matmul(a, b, exact):
    precision = lax.Precision.HIGHEST if exact else lax.Precision.DEFAULT
    return jnp.dot(a, b, precision=precision, preferred_element_type=F32)


def add_face(column, plane, x, odd):
    slot = (2 * x - jnp.where(odd, 1, 0)) % HZ
    return jnp.where(lane_of() % HZ == slot, pltpu.roll(plane, 2 * x, 1), column)


def fetch(pairs, arrived):
    copies = [pltpu.make_async_copy(source, target, arrived.at[i]) for i, (source, target) in enumerate(pairs)]
    for copy in copies:
        copy.start()
    return copies


def split_sites(mixed, odd, low):
    lower, upper = mixed[:HY], mixed[HY:]
    lower_turned, upper_turned = roll(lower, HZ), roll(upper, HZ)
    even_site = jnp.where(low, jnp.where(odd, lower_turned, lower), jnp.where(odd, upper, upper_turned))
    odd_site = jnp.where(low, jnp.where(odd, lower, lower_turned), jnp.where(odd, upper_turned, upper))
    return even_site, odd_site


def spins_kernel(where, occ_hbm, spin, x_one, x_two, y_one, y_two, zed, occ, arrived):
    copies = fetch([(occ_hbm.at[pl.ds(c * CHUNK, CHUNK)], occ.at[pl.ds(c * CHUNK, CHUNK)]) for c in range(BX // CHUNK)], arrived)
    lane = lane_of()
    wide = shuffle_matrix(False)
    columns = [jnp.zeros((HY, BZ), F32)] * 2
    for x in range(BX):
        if x % CHUNK == 0:
            copies[x // CHUNK].wait()
        planes = split_sites(matmul(2.0 * occ[x].astype(F32) - 1.0, wide, False), odd_row(x), lane < HZ)
        for p, plane in enumerate(planes):
            spin[p, x + 1, :HY] = plane
            columns[p] = add_face(columns[p], plane, x, odd_row(x + p))
    for p in range(2):
        x_one[p] = spin[p, far_or_near(where[1], BX, 1), :HY]
        x_two[p] = spin[p, far_or_near(where[1], 1, BX), :HY]
        one, two = far_or_near(where[2], HY - 1, 0), far_or_near(where[2], 0, HY - 1)
        for x in range(BX):
            y_one[p, x : x + 1] = spin[p, x + 1, pl.ds(one, 1)]
            y_two[p, x : x + 1] = spin[p, x + 1, pl.ds(two, 1)]
        zed[p] = columns[p]


def shuffled(value, wide):
    high = value.astype(BF16)
    rest = value - high.astype(F32)
    middle = rest.astype(BF16)
    low = (rest - middle.astype(F32)).astype(BF16)
    rows = value.shape[0]
    parts = jnp.dot(jnp.concatenate([high, middle, low], axis=0), wide, preferred_element_type=F32)
    return parts[:rows] + parts[rows : 2 * rows] + parts[2 * rows :]


def fields_kernel(field_hbm, attempt_hbm, uniforms, h, a, v, field, attempt, raw, arrived):
    copies = fetch([(field_hbm, field), (attempt_hbm, attempt), (uniforms.at[0], raw)], arrived)
    low = lane_of() < HZ
    wide = shuffle_matrix(False).astype(BF16)
    for copy in copies:
        copy.wait()

    @pl.loop(0, BX // UNROLL)
    def _(i):
        for j in range(UNROLL):
            x = i * UNROLL + j
            h[0, x], h[1, x] = split_sites(shuffled(field[x], wide), odd_row(j), low)
            even_site, odd_site = split_sites(shuffled(attempt[x], wide), odd_row(j), low)
            a[0, x], a[1, x] = even_site, odd_site
            v[x] = merged(raw[x]) / even_site


def merged(draws):
    return jnp.concatenate([draws[:HY], draws[HY:]], axis=1)


def draw_kernel(act, where, uniforms, a, v, raw, arrived):
    (copy,) = fetch([(uniforms.at[where[0]], raw)], arrived)
    copy.wait()

    @pl.loop(0, BX // UNROLL)
    def _(i):
        for j in range(UNROLL):
            x = i * UNROLL + j
            v[x] = merged(raw[x]) / a[act, x]


def far_or_near(even, far, near):
    return jnp.where(even == 1, far, near)


def pick(even, first, second):
    return jnp.where(even == 1, first, second)


def side_halo(where, one, two):
    return jnp.where(lane_of(BX) < HZ, pick(where[2], one, two), pick(where[2], two, one))


def column_halo(where, one, two):
    return jnp.where(lane_of() % 2 == 1, pick(where[3], two, one), pick(where[3], one, two))


def flip_of(total, half):
    ratio = total / half
    square = ratio * ratio
    return lambda odds: 1.0 - 2.0 / (1.0 + odds * square)


def eighth(value):
    return value[0:8] + value[8:16] + value[16:24] + value[24:32]


def advance(k, p, half, gathered, halo, spin, side, column, odds, gain, h, energy, fields, clock):
    rows = gathered.shape[0]
    parts = gathered[...]
    while rows % 16 == 0:
        rows //= 2
        parts = parts[:rows] + parts[rows:]
    total = jnp.sum(jnp.sum(parts, axis=0, keepdims=True), axis=1, keepdims=True)
    flip = flip_of(total, half)
    elapsed = clock[1:2, :] + half / total
    clock[1:2, :] = elapsed
    clock[0:1, :] = jnp.where(lane_of(1) == k - 1, elapsed, clock[0:1, :])
    of_gain = jnp.zeros((HY, BZ), F32)
    of_field = jnp.zeros((HY, BZ), F32)

    def step(i, carry):
        of_gain, of_field = carry
        for j in range(UNROLL):
            x = i * UNROLL + j
            new = spin[p, x + 1, :HY] * flip(odds[x])
            spin[p, x + 1, :HY] = new
            of_gain = of_gain + new * gain[x]
            of_field = of_field + new * h[p, x]
        return of_gain, of_field

    of_gain, of_field = lax.fori_loop(0, BX // UNROLL, step, (of_gain, of_field))
    fields[p] = eighth(of_field)
    energy[k - 1] = -eighth(of_gain) - fields[1 - p]
    if halo is None:
        return
    where, x_one, x_two, y_one, y_two, z_one, z_two = halo
    one, two = far_or_near(where[1], BX + 1, 0), far_or_near(where[1], 0, BX + 1)
    spin[p, one, :HY] = spin[p, one, :HY] * flip(x_one[...])
    spin[p, two, :HY] = spin[p, two, :HY] * flip(x_two[...])
    side[p] = side[p] * flip(side_halo(where, y_one[...], y_two[...]))
    column[p] = column[p] * flip(column_halo(where, z_one[...], z_two[...]))


def rates(act, where, spin, side, column, odds, gain, h, a, v, x_one, x_two, y_one, y_two, zed, sent):
    p = 1 - act
    lane = lane_of()
    one_row = lane_of(1)
    for x in range(BX):
        first, last = spin[p, x + 1, :1], spin[p, x + 1, HY - 1 : HY]
        beyond = side[p, x : x + 1]
        spin[p, x + 1, HY + 1 : HY + 2] = roll(jnp.where(one_row < HZ, last, beyond), HZ)
        spin[p, x + 1, HY : HY + 1] = roll(jnp.where(one_row < HZ, beyond, first), HZ)
    ends = column[p]
    top = lax.broadcasted_iota(jnp.int32, (HY, BZ), 0) == 0

    def step(i, carry):
        packed, summed = carry
        for j in range(UNROLL):
            x = i * UNROLL + j
            odd = odd_row(j + act)
            here = spin[p, x + 1, :HY]
            joined = jnp.where(lane % HZ == jnp.where(odd, 0, HZ - 1), pltpu.roll(ends, (BZ + HZ - 2 * x) % BZ, 1), here)
            turned = jnp.where(odd, roll(joined, -1), roll(joined, 1))
            beside = spin[p, x, :HY] + spin[p, x + 2, :HY]
            beside = beside + jnp.where(top, spin[p, x + 1, HY + 1 : HY + 2], pltpu.roll(here, 1, 0)) + spin[p, x + 1, 1 : HY + 1]
            beside = beside + here + turned
            g = h[act, x] - 0.5 * beside
            gain[x] = g
            grown = 1.0 + jnp.exp(2.0 * spin[act, x + 1, :HY] * g)
            summed = summed + a[act, x] / grown
            root = v[x] * grown
            square = root * root
            odds[x] = square
            packed = add_face(packed, square, x, odd)
        return packed, summed

    packed, summed = lax.fori_loop(0, BX // UNROLL, step, (jnp.zeros((HY, BZ), F32), jnp.zeros((HY, BZ), F32)))
    x_one[...] = odds[far_or_near(where[1], BX - 1, 0)]
    x_two[...] = odds[far_or_near(where[1], 0, BX - 1)]
    one, two = far_or_near(where[2], HY - 1, 0), far_or_near(where[2], 0, HY - 1)
    for x in range(BX):
        y_one[x : x + 1] = odds[x, pl.ds(one, 1)]
        y_two[x : x + 1] = odds[x, pl.ds(two, 1)]
    zed[...] = packed
    sent[...] = jnp.broadcast_to(jnp.sum(summed, axis=0, keepdims=True), sent.shape)


def first_kernel(
    where, from_x_one, from_x_two, from_y_one, from_y_two, from_z_one, from_z_two, h, a, v, spin_in,
    spin, side, column, energy, fields, clock, odds, gain, x_one, x_two, y_one, y_two, zed, sent,
):
    for p in range(2):
        spin[p, far_or_near(where[1], BX + 1, 0), :HY] = from_x_one[p]
        spin[p, far_or_near(where[1], 0, BX + 1), :HY] = from_x_two[p]
        side[p] = side_halo(where, from_y_one[p], from_y_two[p])
        column[p] = column_halo(where, from_z_one[p], from_z_two[p])
    of_field = jnp.zeros((HY, BZ), F32)
    for x in range(BX):
        of_field = of_field + spin[1, x + 1, :HY] * h[1, x]
    fields[0] = jnp.zeros((8, BZ), F32)
    fields[1] = eighth(of_field)
    energy[...] = jnp.zeros(energy.shape, F32)
    clock[...] = jnp.zeros(clock.shape, F32)
    rates(0, where, spin, side, column, odds, gain, h, a, v, x_one, x_two, y_one, y_two, zed, sent)


def section_kernel(
    act, half, where, gathered, from_x_one, from_x_two, from_y_one, from_y_two, from_z_one, from_z_two, h, a, v,
    spin_in, side_in, column_in, energy_in, fields_in, clock_in, odds_in, gain_in,
    spin, side, column, energy, fields, clock, odds, gain, x_one, x_two, y_one, y_two, zed, sent,
):
    k = where[0]
    halo = (where, from_x_one, from_x_two, from_y_one, from_y_two, from_z_one, from_z_two)
    advance(k, 1 - act, half, gathered, halo, spin, side, column, odds, gain, h, energy, fields, clock)
    rates(act, where, spin, side, column, odds, gain, h, a, v, x_one, x_two, y_one, y_two, zed, sent)


def last_kernel(
    half, gathered, h, odds, gain, spin_in, energy_in, fields_in, clock_in,
    spin, energy, fields, clock, sent,
):
    advance(SECTIONS, (SECTIONS - 1) % 2, half, gathered, None, spin, None, None, odds, gain, h, energy, fields, clock)
    row = jnp.zeros((1, BZ), F32)
    for k in range(SECTIONS):
        value = jnp.sum(jnp.sum(energy[k], axis=0, keepdims=True), axis=1, keepdims=True)
        row = jnp.where(lane_of(1) == k, value, row)
    sent[...] = jnp.broadcast_to(row, sent.shape)


def unpack_kernel(spin, out):
    low = lane_of() < HZ
    narrow = shuffle_matrix(True)
    for x in range(BX):
        even_site, odd_site = spin[0, x + 1, :HY], spin[1, x + 1, :HY]
        odd = odd_row(x)
        even_z, odd_z = jnp.where(odd, odd_site, even_site), jnp.where(odd, even_site, odd_site)
        lower = jnp.where(low, even_z, roll(odd_z, HZ))
        upper = jnp.where(low, roll(even_z, HZ), odd_z)
        out[x, :HY] = matmul(lower, narrow, True)
        out[x, HY:] = matmul(upper, narrow, True)


def history_kernel(sites, gathered, clock, out):
    row = jnp.sum(gathered[...], axis=0, keepdims=True) / sites
    out[0:1, :] = row[:, :SECTIONS]
    out[1:2, :] = clock[0:1, :SECTIONS]


def call(kernel, inputs, outputs, aliases=None, far=(), far_out=(), scratch=(), flops=1000000):
    held, away = pl.BlockSpec(memory_space=pltpu.VMEM), pl.BlockSpec(memory_space=pltpu.HBM)
    inputs = [pltpu.with_memory_space_constraint(x, pltpu.HBM) if i in far else x for i, x in enumerate(inputs)]
    scalar = pl.BlockSpec(memory_space=pltpu.SMEM)
    return pl.pallas_call(
        kernel,
        out_shape=[pltpu.HBM(shape, F32) if i in far_out else jax.ShapeDtypeStruct(shape, F32) for i, shape in enumerate(outputs)],
        in_specs=[away if i in far else scalar if x.shape == (4,) else held for i, x in enumerate(inputs)],
        out_specs=[away if i in far_out else held for i in range(len(outputs))],
        input_output_aliases=aliases or {},
        scratch_shapes=scratch,
        compiler_params=pltpu.CompilerParams(vmem_limit_bytes=24 * 1024 * 1024),
        cost_estimate=pl.CostEstimate(flops=flops, bytes_accessed=1000000, transcendentals=0),
    )(*inputs)


def swap(x_one, x_two, y_one, y_two, z_one, z_two):
    got = []
    for axis, one, two in (("gx", x_one, x_two), ("gy", y_one, y_two), ("gz", z_one, z_two)):
        count = lax.axis_size(axis)
        for block, shift in ((one, 0), (two, 1)):
            pairs = [(i, (i + (1 if i % 2 == shift else -1)) % count) for i in range(count)]
            got.append(lax.ppermute(block, axis, pairs))
    return got


def spread(sent):
    return lax.all_to_all(sent, AXES, 0, 0, tiled=True)


def body(occupancy, site_field, attempt_rate, uniforms):
    devices = lax.axis_size(AXES)
    sites = float(BX * BY * BZ * devices)
    half = sites / 2.0
    tile = (HY, BZ)
    spin_shape = (2, BX + 2, PITCH, BZ)
    block = (BX, *tile)
    faces = [tile, tile, (BX, BZ), (BX, BZ), tile]
    state = [spin_shape, (2, BX, BZ), (2, *tile), (SECTIONS, 8, BZ), (2, 8, BZ), (8, BZ), block, block]
    sent_shape = (devices, BZ)
    dma = pltpu.SemaphoreType.DMA
    evens = [1 - lax.axis_index(axis) % 2 for axis in AXES]

    def where(k):
        return jnp.stack([jnp.asarray(k, jnp.int32), *evens]).astype(jnp.int32)

    spin, *sides = call(
        spins_kernel, (where(0), occupancy), [spin_shape] + [(2, *face) for face in faces], far=(1,),
        scratch=[pltpu.VMEM((BX, BY, BZ), jnp.int32), dma((BX // CHUNK,))],
    )
    halo = swap(*sides, sides[-1])
    brick = pltpu.VMEM((BX, BY, BZ), F32)
    drawn = pltpu.VMEM((BX, BY, HZ), F32)
    h, a, v = call(
        fields_kernel, (site_field, attempt_rate, uniforms), [(2, *block), (2, *block), block],
        far=(0, 1, 2), scratch=[brick, brick, drawn, dma((3,))],
    )
    carried = call(first_kernel, (where(0), *halo, h, a, v, spin), state + faces + [sent_shape], {10: 0})

    def section(k, act, carried):
        *kept, x_one, x_two, y_one, y_two, zed, sent = carried
        gathered = spread(sent)
        halo = swap(x_one, x_two, y_one, y_two, zed, zed)
        (v,) = call(
            functools.partial(draw_kernel, act), (where(k), uniforms, a), [block],
            far=(1,), scratch=[drawn, dma((1,))],
        )
        return call(
            functools.partial(section_kernel, act, half),
            (where(k), gathered, *halo, h, a, v, *kept), state + faces + [sent_shape],
            {11 + i: i for i in range(len(state))},
        )

    def pair(i, carried):
        return section(2 * i + 2, 0, section(2 * i + 1, 1, carried))

    carried = lax.fori_loop(0, SECTIONS // 2 - 1, pair, carried)
    carried = section(SECTIONS - 1, 1, carried)
    spin, _, _, energy, fields, clock, odds, gain = carried[: len(state)]
    gathered = spread(carried[-1])
    spin, energy, fields, clock, sent = call(
        functools.partial(last_kernel, half),
        (gathered, h, odds, gain, spin, energy, fields, clock),
        [spin_shape, state[3], state[4], state[5], sent_shape], {4: 0, 5: 1, 6: 2, 7: 3},
    )
    gathered = spread(sent)
    (final,) = call(unpack_kernel, (spin,), [(BX, BY, BZ)])
    (history,) = call(functools.partial(history_kernel, sites), (gathered, clock), [(2, SECTIONS)])
    return final, history


def solution(mesh):
    return jax.shard_map(
        body,
        mesh=mesh,
        in_specs=(P(*AXES), P(*AXES), P(*AXES), P(None, *AXES)),
        out_specs=(P(*AXES), P()),
        check_vma=False,
    )
```

```python
import functools

import jax
import jax.numpy as jnp
from jax import lax
from jax.experimental import pallas as pl
from jax.experimental.pallas import tpu as pltpu
from jax.sharding import PartitionSpec as P


SECTIONS = 8
AXES = ("gx", "gy", "gz")
BX, BY, BZ = 16, 64, 128
HY, HZ = BY // 2, BZ // 2
UNROLL = 16
CHUNK = 4
PITCH = HY + 8
F32, BF16 = jnp.float32, jnp.bfloat16


def lane_of(rows=HY):
    return lax.broadcasted_iota(jnp.int32, (rows, BZ), 1)


def odd_row(shift, rows=HY):
    return (lax.broadcasted_iota(jnp.int32, (rows, BZ), 0) + shift) % 2 == 1


def roll(value, shift):
    shift = shift % BZ
    return value if shift == 0 else pltpu.roll(value, shift, 1)


def shuffle_matrix(transposed):
    major = lax.broadcasted_iota(jnp.int32, (BZ, BZ), 1 if transposed else 0)
    minor = lax.broadcasted_iota(jnp.int32, (BZ, BZ), 0 if transposed else 1)
    return (minor == major // 2 + HZ * (major % 2)).astype(F32)


def matmul(a, b, exact):
    precision = lax.Precision.HIGHEST if exact else lax.Precision.DEFAULT
    return jnp.dot(a, b, precision=precision, preferred_element_type=F32)


def add_face(column, plane, x, odd):
    slot = (2 * x - jnp.where(odd, 1, 0)) % HZ
    return jnp.where(lane_of() % HZ == slot, pltpu.roll(plane, 2 * x, 1), column)


def fetch(pairs, arrived):
    copies = [pltpu.make_async_copy(source, target, arrived.at[i]) for i, (source, target) in enumerate(pairs)]
    for copy in copies:
        copy.start()
    return copies


def split_sites(mixed, odd, low):
    lower, upper = mixed[:HY], mixed[HY:]
    lower_turned, upper_turned = roll(lower, HZ), roll(upper, HZ)
    even_site = jnp.where(low, jnp.where(odd, lower_turned, lower), jnp.where(odd, upper, upper_turned))
    odd_site = jnp.where(low, jnp.where(odd, lower, lower_turned), jnp.where(odd, upper_turned, upper))
    return even_site, odd_site


def spins_kernel(where, occ_hbm, spin, x_one, x_two, y_one, y_two, zed, occ, arrived):
    copies = fetch([(occ_hbm.at[pl.ds(c * CHUNK, CHUNK)], occ.at[pl.ds(c * CHUNK, CHUNK)]) for c in range(BX // CHUNK)], arrived)
    lane = lane_of()
    wide = shuffle_matrix(False)
    columns = [jnp.zeros((HY, BZ), F32)] * 2
    for x in range(BX):
        if x % CHUNK == 0:
            copies[x // CHUNK].wait()
        planes = split_sites(matmul(2.0 * occ[x].astype(F32) - 1.0, wide, False), odd_row(x), lane < HZ)
        for p, plane in enumerate(planes):
            spin[p, x + 1, :HY] = plane
            columns[p] = add_face(columns[p], plane, x, odd_row(x + p))
    for p in range(2):
        x_one[p] = spin[p, far_or_near(where[1], BX, 1), :HY]
        x_two[p] = spin[p, far_or_near(where[1], 1, BX), :HY]
        one, two = far_or_near(where[2], HY - 1, 0), far_or_near(where[2], 0, HY - 1)
        for x in range(BX):
            y_one[p, x : x + 1] = spin[p, x + 1, pl.ds(one, 1)]
            y_two[p, x : x + 1] = spin[p, x + 1, pl.ds(two, 1)]
        zed[p] = columns[p]


def shuffled(value, wide):
    high = value.astype(BF16)
    rest = value - high.astype(F32)
    middle = rest.astype(BF16)
    low = (rest - middle.astype(F32)).astype(BF16)
    rows = value.shape[0]
    parts = jnp.dot(jnp.concatenate([high, middle, low], axis=0), wide, preferred_element_type=F32)
    return parts[:rows] + parts[rows : 2 * rows] + parts[2 * rows :]


def fields_kernel(field_hbm, attempt_hbm, uniforms, h, a, v, field, attempt, raw, arrived):
    copies = fetch([(field_hbm, field), (attempt_hbm, attempt), (uniforms.at[0], raw)], arrived)
    low = lane_of() < HZ
    wide = shuffle_matrix(False).astype(BF16)
    for copy in copies:
        copy.wait()

    @pl.loop(0, BX // UNROLL)
    def _(i):
        for j in range(UNROLL):
            x = i * UNROLL + j
            h[0, x], h[1, x] = split_sites(shuffled(field[x], wide), odd_row(j), low)
            even_site, odd_site = split_sites(shuffled(attempt[x], wide), odd_row(j), low)
            a[0, x], a[1, x] = even_site, odd_site
            v[x] = merged(raw[x]) / even_site


def merged(draws):
    return jnp.concatenate([draws[:HY], draws[HY:]], axis=1)


def draw_kernel(act, where, uniforms, a, v, raw, arrived):
    (copy,) = fetch([(uniforms.at[where[0]], raw)], arrived)
    copy.wait()

    @pl.loop(0, BX // UNROLL)
    def _(i):
        for j in range(UNROLL):
            x = i * UNROLL + j
            v[x] = merged(raw[x]) / a[act, x]


def far_or_near(even, far, near):
    return jnp.where(even == 1, far, near)


def pick(even, first, second):
    return jnp.where(even == 1, first, second)


def side_halo(where, one, two):
    return jnp.where(lane_of(BX) < HZ, pick(where[2], one, two), pick(where[2], two, one))


def column_halo(where, one, two):
    return jnp.where(lane_of() % 2 == 1, pick(where[3], two, one), pick(where[3], one, two))


def flip_of(total, half):
    ratio = total / half
    square = ratio * ratio
    return lambda odds: 1.0 - 2.0 / (1.0 + odds * square)


def eighth(value):
    return value[0:8] + value[8:16] + value[16:24] + value[24:32]


def advance(k, p, half, gathered, halo, spin, side, column, odds, gain, h, energy, fields, clock):
    rows = gathered.shape[0]
    parts = gathered[...]
    while rows % 16 == 0:
        rows //= 2
        parts = parts[:rows] + parts[rows:]
    total = jnp.sum(jnp.sum(parts, axis=0, keepdims=True), axis=1, keepdims=True)
    flip = flip_of(total, half)
    elapsed = clock[1:2, :] + half / total
    clock[1:2, :] = elapsed
    clock[0:1, :] = jnp.where(lane_of(1) == k - 1, elapsed, clock[0:1, :])
    of_gain = jnp.zeros((HY, BZ), F32)
    of_field = jnp.zeros((HY, BZ), F32)

    def step(i, carry):
        of_gain, of_field = carry
        for j in range(UNROLL):
            x = i * UNROLL + j
            new = spin[p, x + 1, :HY] * flip(odds[x])
            spin[p, x + 1, :HY] = new
            of_gain = of_gain + new * gain[x]
            of_field = of_field + new * h[p, x]
        return of_gain, of_field

    of_gain, of_field = lax.fori_loop(0, BX // UNROLL, step, (of_gain, of_field))
    fields[p] = eighth(of_field)
    energy[k - 1] = -eighth(of_gain) - fields[1 - p]
    if halo is None:
        return
    where, x_one, x_two, y_one, y_two, z_one, z_two = halo
    one, two = far_or_near(where[1], BX + 1, 0), far_or_near(where[1], 0, BX + 1)
    spin[p, one, :HY] = spin[p, one, :HY] * flip(x_one[...])
    spin[p, two, :HY] = spin[p, two, :HY] * flip(x_two[...])
    side[p] = side[p] * flip(side_halo(where, y_one[...], y_two[...]))
    column[p] = column[p] * flip(column_halo(where, z_one[...], z_two[...]))


def rates(act, where, spin, side, column, odds, gain, h, a, v, x_one, x_two, y_one, y_two, zed, sent, row, leaves):
    p = 1 - act
    lane = lane_of()
    one_row = lane_of(1)
    for x in range(BX):
        first, last = spin[p, x + 1, :1], spin[p, x + 1, HY - 1 : HY]
        beyond = side[p, x : x + 1]
        spin[p, x + 1, HY + 1 : HY + 2] = roll(jnp.where(one_row < HZ, last, beyond), HZ)
        spin[p, x + 1, HY : HY + 1] = roll(jnp.where(one_row < HZ, beyond, first), HZ)
    ends = column[p]
    top = lax.broadcasted_iota(jnp.int32, (HY, BZ), 0) == 0

    def step(i, carry):
        summed = carry
        for j in range(UNROLL):
            x = i * UNROLL + j
            odd = odd_row(j + act)
            here = spin[p, x + 1, :HY]
            joined = jnp.where(lane % HZ == jnp.where(odd, 0, HZ - 1), pltpu.roll(ends, (BZ + HZ - 2 * x) % BZ, 1), here)
            turned = jnp.where(odd, roll(joined, -1), roll(joined, 1))
            beside = spin[p, x, :HY] + spin[p, x + 2, :HY]
            beside = beside + jnp.where(top, spin[p, x + 1, HY + 1 : HY + 2], pltpu.roll(here, 1, 0)) + spin[p, x + 1, 1 : HY + 1]
            beside = beside + here + turned
            g = h[act, x] - 0.5 * beside
            gain[x] = g
            grown = 1.0 + jnp.exp(2.0 * spin[act, x + 1, :HY] * g)
            summed = summed + a[act, x] / grown
            odds[x] = grown
        return summed

    summed = lax.fori_loop(0, BX // UNROLL, step, jnp.zeros((HY, BZ), F32))
    row[...] = jnp.broadcast_to(jnp.sum(summed, axis=0, keepdims=True), row.shape)
    leaving = pltpu.make_async_copy(row, sent, leaves)
    leaving.start()
    packed = jnp.zeros((HY, BZ), F32)
    for x in range(BX):
        root = v[x] * odds[x]
        square = root * root
        odds[x] = square
        packed = add_face(packed, square, x, odd_row(x + act))
    x_one[...] = odds[far_or_near(where[1], BX - 1, 0)]
    x_two[...] = odds[far_or_near(where[1], 0, BX - 1)]
    one, two = far_or_near(where[2], HY - 1, 0), far_or_near(where[2], 0, HY - 1)
    for x in range(BX):
        y_one[x : x + 1] = odds[x, pl.ds(one, 1)]
        y_two[x : x + 1] = odds[x, pl.ds(two, 1)]
    zed[...] = packed
    leaving.wait()


def first_kernel(
    where, from_x_one, from_x_two, from_y_one, from_y_two, from_z_one, from_z_two, h, a, v, spin_in,
    spin, side, column, energy, fields, clock, odds, gain, x_one, x_two, y_one, y_two, zed, sent, row, leaves,
):
    for p in range(2):
        spin[p, far_or_near(where[1], BX + 1, 0), :HY] = from_x_one[p]
        spin[p, far_or_near(where[1], 0, BX + 1), :HY] = from_x_two[p]
        side[p] = side_halo(where, from_y_one[p], from_y_two[p])
        column[p] = column_halo(where, from_z_one[p], from_z_two[p])
    of_field = jnp.zeros((HY, BZ), F32)
    for x in range(BX):
        of_field = of_field + spin[1, x + 1, :HY] * h[1, x]
    fields[0] = jnp.zeros((8, BZ), F32)
    fields[1] = eighth(of_field)
    energy[...] = jnp.zeros(energy.shape, F32)
    clock[...] = jnp.zeros(clock.shape, F32)
    rates(0, where, spin, side, column, odds, gain, h, a, v, x_one, x_two, y_one, y_two, zed, sent, row, leaves)


def section_kernel(
    act, half, where, gathered, from_x_one, from_x_two, from_y_one, from_y_two, from_z_one, from_z_two, h, a, v,
    spin_in, side_in, column_in, energy_in, fields_in, clock_in, odds_in, gain_in,
    spin, side, column, energy, fields, clock, odds, gain, x_one, x_two, y_one, y_two, zed, sent, row, leaves,
):
    k = where[0]
    halo = (where, from_x_one, from_x_two, from_y_one, from_y_two, from_z_one, from_z_two)
    advance(k, 1 - act, half, gathered, halo, spin, side, column, odds, gain, h, energy, fields, clock)
    rates(act, where, spin, side, column, odds, gain, h, a, v, x_one, x_two, y_one, y_two, zed, sent, row, leaves)


def last_kernel(
    half, gathered, h, odds, gain, spin_in, energy_in, fields_in, clock_in,
    spin, energy, fields, clock, sent,
):
    advance(SECTIONS, (SECTIONS - 1) % 2, half, gathered, None, spin, None, None, odds, gain, h, energy, fields, clock)
    row = jnp.zeros((1, BZ), F32)
    for k in range(SECTIONS):
        value = jnp.sum(jnp.sum(energy[k], axis=0, keepdims=True), axis=1, keepdims=True)
        row = jnp.where(lane_of(1) == k, value, row)
    sent[...] = jnp.broadcast_to(row, sent.shape)


def unpack_kernel(spin, out):
    low = lane_of() < HZ
    narrow = shuffle_matrix(True)
    for x in range(BX):
        even_site, odd_site = spin[0, x + 1, :HY], spin[1, x + 1, :HY]
        odd = odd_row(x)
        even_z, odd_z = jnp.where(odd, odd_site, even_site), jnp.where(odd, even_site, odd_site)
        lower = jnp.where(low, even_z, roll(odd_z, HZ))
        upper = jnp.where(low, roll(even_z, HZ), odd_z)
        out[x, :HY] = matmul(lower, narrow, True)
        out[x, HY:] = matmul(upper, narrow, True)


def history_kernel(sites, gathered, clock, out):
    row = jnp.sum(gathered[...], axis=0, keepdims=True) / sites
    out[0:1, :] = row[:, :SECTIONS]
    out[1:2, :] = clock[0:1, :SECTIONS]


def call(kernel, inputs, outputs, aliases=None, far=(), far_out=(), scratch=(), flops=1000000):
    held, away = pl.BlockSpec(memory_space=pltpu.VMEM), pl.BlockSpec(memory_space=pltpu.HBM)
    inputs = [pltpu.with_memory_space_constraint(x, pltpu.HBM) if i in far else x for i, x in enumerate(inputs)]
    scalar = pl.BlockSpec(memory_space=pltpu.SMEM)
    return pl.pallas_call(
        kernel,
        out_shape=[pltpu.HBM(shape, F32) if i in far_out else jax.ShapeDtypeStruct(shape, F32) for i, shape in enumerate(outputs)],
        in_specs=[away if i in far else scalar if x.shape == (4,) else held for i, x in enumerate(inputs)],
        out_specs=[away if i in far_out else held for i in range(len(outputs))],
        input_output_aliases=aliases or {},
        scratch_shapes=scratch,
        compiler_params=pltpu.CompilerParams(vmem_limit_bytes=24 * 1024 * 1024),
        cost_estimate=pl.CostEstimate(flops=flops, bytes_accessed=1000000, transcendentals=0),
    )(*inputs)


def swap(x_one, x_two, y_one, y_two, z_one, z_two):
    got = []
    for axis, one, two in (("gx", x_one, x_two), ("gy", y_one, y_two), ("gz", z_one, z_two)):
        count = lax.axis_size(axis)
        for block, shift in ((one, 0), (two, 1)):
            pairs = [(i, (i + (1 if i % 2 == shift else -1)) % count) for i in range(count)]
            got.append(lax.ppermute(block, axis, pairs))
    return got


def spread(sent):
    return lax.all_to_all(sent, AXES, 0, 0, tiled=True)


def body(occupancy, site_field, attempt_rate, uniforms):
    devices = lax.axis_size(AXES)
    sites = float(BX * BY * BZ * devices)
    half = sites / 2.0
    tile = (HY, BZ)
    spin_shape = (2, BX + 2, PITCH, BZ)
    block = (BX, *tile)
    faces = [tile, tile, (BX, BZ), (BX, BZ), tile]
    state = [spin_shape, (2, BX, BZ), (2, *tile), (SECTIONS, 8, BZ), (2, 8, BZ), (8, BZ), block, block]
    sent_shape = (devices, BZ)
    dma = pltpu.SemaphoreType.DMA
    evens = [1 - lax.axis_index(axis) % 2 for axis in AXES]

    def where(k):
        return jnp.stack([jnp.asarray(k, jnp.int32), *evens]).astype(jnp.int32)

    spin, *sides = call(
        spins_kernel, (where(0), occupancy), [spin_shape] + [(2, *face) for face in faces], far=(1,),
        scratch=[pltpu.VMEM((BX, BY, BZ), jnp.int32), dma((BX // CHUNK,))],
    )
    halo = swap(*sides, sides[-1])
    brick = pltpu.VMEM((BX, BY, BZ), F32)
    drawn = pltpu.VMEM((BX, BY, HZ), F32)
    h, a, v = call(
        fields_kernel, (site_field, attempt_rate, uniforms), [(2, *block), (2, *block), block],
        far=(0, 1, 2), scratch=[brick, brick, drawn, dma((3,))],
    )
    carried = call(
        first_kernel, (where(0), *halo, h, a, v, spin), state + faces + [sent_shape], {10: 0},
        far_out=(len(state) + len(faces),), scratch=[pltpu.VMEM(sent_shape, F32), dma],
    )

    def section(k, act, carried):
        *kept, x_one, x_two, y_one, y_two, zed, sent = carried
        gathered = spread(sent)
        halo = swap(x_one, x_two, y_one, y_two, zed, zed)
        (v,) = call(
            functools.partial(draw_kernel, act), (where(k), uniforms, a), [block],
            far=(1,), scratch=[drawn, dma((1,))],
        )
        return call(
            functools.partial(section_kernel, act, half),
            (where(k), gathered, *halo, h, a, v, *kept), state + faces + [sent_shape],
            {11 + i: i for i in range(len(state))}, far_out=(len(state) + len(faces),),
            scratch=[pltpu.VMEM(sent_shape, F32), dma],
        )

    def pair(i, carried):
        return section(2 * i + 2, 0, section(2 * i + 1, 1, carried))

    carried = lax.fori_loop(0, SECTIONS // 2 - 1, pair, carried)
    carried = section(SECTIONS - 1, 1, carried)
    spin, _, _, energy, fields, clock, odds, gain = carried[: len(state)]
    gathered = spread(carried[-1])
    spin, energy, fields, clock, sent = call(
        functools.partial(last_kernel, half),
        (gathered, h, odds, gain, spin, energy, fields, clock),
        [spin_shape, state[3], state[4], state[5], sent_shape], {4: 0, 5: 1, 6: 2, 7: 3},
    )
    gathered = spread(sent)
    (final,) = call(unpack_kernel, (spin,), [(BX, BY, BZ)])
    (history,) = call(functools.partial(history_kernel, sites), (gathered, clock), [(2, SECTIONS)])
    return final, history


def solution(mesh):
    return jax.shard_map(
        body,
        mesh=mesh,
        in_specs=(P(*AXES), P(*AXES), P(*AXES), P(None, *AXES)),
        out_specs=(P(*AXES), P()),
        check_vma=False,
    )
```
